32 devices in a mesh: expert: 4 (over y, core), shard: 8 (over z, x).
Axes of the slice: x: 2, y: 2, z: 4, core: 2. Of those that a mesh axis runs over, the one named last changes fastest.
Arguments:
- activations: bfloat16 [4, 8, 96, 2048], P('expert', 'shard'), may hold values from -6 to 6
- out_grads: bfloat16 [4, 8, 96, 7168], P('expert', 'shard'), may hold values from -6 to 6
- next_inputs: bfloat16 [4, 8, 96, 2048], P('expert', 'shard'), may hold values from -6 to 6
- counts: int32 [4, 8], P('expert', 'shard'), may hold values from 1 to 96, as said below
- master: float32 [4, 8, 2048, 896], P('expert', 'shard'), may hold values from -0.125 to 0.125
- moment: bfloat16 [4, 8, 2048, 896], P('expert', 'shard'), may hold values from -6 to 6
- second: bfloat16 [4, 8, 2048, 896], P('expert', 'shard'), may hold values from 0.099609375 to 4
Outputs:
- master_new: float32 [4, 8, 2048, 896], P('expert', 'shard')
- moment_new: bfloat16 [4, 8, 2048, 896], P('expert', 'shard')
- second_new: bfloat16 [4, 8, 2048, 896], P('expert', 'shard')
- projected: bfloat16 [4, 8, 96, 7168], P('expert', 'shard')
The draws below stay inside these ranges and needn't reach their ends.
Inputs may be any that keep to these rules, and one draw needn't show every extreme that they name: counts[e, s] of the 96 slots of expert e from shard s hold tokens, the leading ones; the rest are padding.
All inputs are finite; a program needn't handle non-finite values.
Results may differ from the reference program's by a relative error of at most 0.00055.
The reference program's roundings to bfloat16 on the way count: a program that leaves them out, or rounds other values in their place, can miss the bound.
Values may be sent and summed in bfloat16 or wider, within the bound.
A program may use at most 192 MiB of HBM per device.

```python
import math
import jax
import jax.numpy as jnp
from jax import lax

D = 2048
FF = 7168
CAP = 96
EXPERTS = 4
GRID_R = 1
GRID_C = 8
D_BLK = 2048
F_BLK = 896
N_SHARD = 8


def draw_counts(key, part):
    base_key = jax.random.fold_in(key, 7)
    first_key, second_key, third_key, fourth_key = jax.random.split(base_key, 4)
    base = jax.random.randint(first_key, (EXPERTS, N_SHARD), 0, CAP)
    loads = jax.random.randint(second_key, (EXPERTS, 1), 2, 5)
    result = 1 + base * loads // 4
    expert_pick = jax.random.randint(third_key, (), 0, EXPERTS)
    shard_pick = jax.random.randint(fourth_key, (), 0, N_SHARD)
    result = result.at[expert_pick, shard_pick].set(CAP)
    return result.astype(jnp.int32)


def block_scale(rng, dims, cuts, low, high):
    loudness = 1.0
    for axis_at, parts in cuts:
        draws = jax.random.uniform(jax.random.fold_in(jax.random.fold_in(rng, 6), axis_at), (parts,), jnp.float32, low / len(cuts), high / len(cuts))
        loudness = loudness * jnp.repeat(jnp.exp(draws), dims[axis_at] // parts).reshape((-1,) + (1,) * (len(dims) - 1 - axis_at))
    return loudness


def scatter_about(key, dims, width, limit, cuts=(), held_as=jnp.bfloat16):
    values = width * jax.random.normal(key, dims, jnp.float32)
    if cuts:
        values = values * block_scale(key, dims, cuts, -0.22, 0.18)
    return jnp.clip(values, -limit, limit).astype(held_as)


def setup_inputs(seed: int = 0) -> dict:
    key_of = jax.random.split(jax.random.key(seed), 8)
    return {
        "activations": scatter_about(key_of[0], (EXPERTS, N_SHARD, CAP, D), 1.0, 6.0, ((0, 4), (1, 8))),
        "out_grads": scatter_about(key_of[1], (EXPERTS, N_SHARD, CAP, FF), 1.0, 6.0, ((0, 4), (1, 8))),
        "next_inputs": scatter_about(key_of[2], (EXPERTS, N_SHARD, CAP, D), 1.0, 6.0, ((0, 4), (1, 8))),
        "counts": draw_counts(jax.random.fold_in(key_of[7], 71), 0),
        "master": scatter_about(key_of[4], (EXPERTS, N_SHARD, D_BLK, F_BLK), D ** -0.5, 0.125, ((0, 4), (1, 8)), jnp.float32),
        "moment": scatter_about(key_of[5], (EXPERTS, N_SHARD, D_BLK, F_BLK), 1.0, 6.0, ((0, 4), (1, 8))),
        "second": jnp.clip(jnp.exp(math.log(4.0) - 3.6927934 * jax.random.uniform(key_of[6], (EXPERTS, N_SHARD, D_BLK, F_BLK), jnp.float32) ** block_scale(key_of[6], (EXPERTS, N_SHARD, D_BLK, F_BLK), ((0, 4), (1, 8)), -0.2, 0.2)), 0.099609375, 4.0).astype(jnp.bfloat16),
    }


def to_full(tiles):
    return tiles.reshape(EXPERTS, GRID_R, GRID_C, D_BLK, F_BLK).transpose(0, 1, 3, 2, 4).reshape(EXPERTS, D, FF)

def to_tiles(full):
    return full.reshape(EXPERTS, GRID_R, D_BLK, GRID_C, F_BLK).transpose(0, 1, 3, 2, 4).reshape(EXPERTS, N_SHARD, D_BLK, F_BLK)

def expert_grad(couple):
    inputs_here, grads_here = couple
    return jnp.dot(inputs_here.reshape(-1, D).T, grads_here.reshape(-1, FF), preferred_element_type=jnp.float32)

def expert_project(couple):
    inputs_here, matrix = couple
    return jnp.dot(inputs_here.reshape(-1, D), matrix, preferred_element_type=jnp.float32).astype(jnp.bfloat16)

def reference(activations, out_grads, next_inputs, counts, master, moment, second):
    slots = jnp.arange(CAP, dtype=jnp.int32)
    valid = slots[None, None, :] < counts[:, :, None]
    masked = jnp.where(valid[..., None], out_grads, jnp.zeros((), jnp.bfloat16))
    gradient = lax.map(expert_grad, (activations, masked))
    weights = to_full(master)
    first = to_full(moment).astype(jnp.float32)
    later = to_full(second).astype(jnp.float32)
    entries = float(EXPERTS * D * FF)
    grad_rms = jnp.sqrt(jnp.sum(gradient * gradient) / entries + 1e-06)
    clip_factor = jnp.minimum(1.0, 1.0 / grad_rms)
    clipped = clip_factor * gradient
    first_new = 0.9 * first + 0.1 * clipped
    later_new = 0.999 * later + 0.001 * clipped * clipped
    update = first_new / (1.0 - 0.9 ** 10) / (jnp.sqrt(later_new / (1.0 - 0.999 ** 10)) + 1e-06) + 0.01 * weights
    weight_sq = lax.optimization_barrier(jnp.sum(weights * weights, axis=(1, 2)))
    update_sq = lax.optimization_barrier(jnp.sum(update * update, axis=(1, 2)))
    trust_ratio = jnp.sqrt(weight_sq) / (jnp.sqrt(update_sq) + 1e-06)
    weights_new = weights - 0.08 * trust_ratio[:, None, None] * update
    rounded = weights_new.astype(jnp.bfloat16)
    projected = lax.map(expert_project, (next_inputs, rounded)).reshape(EXPERTS, N_SHARD, CAP, FF)
    return (to_tiles(weights_new), to_tiles(first_new).astype(jnp.bfloat16), to_tiles(later_new).astype(jnp.bfloat16), projected)
```

```python
import functools
import jax
import jax.numpy as jnp
from jax import lax
from jax.experimental import pallas as pl
from jax.experimental.pallas import tpu as pltpu
from jax.sharding import PartitionSpec as P

MESH = pl.DeviceIdType.MESH
LANES = 128
SUBLANES = 8


def columns_of(n):
    nx = 1
    while n % (2 * nx) == 0 and 8 * nx * nx <= n:
        nx *= 2
    return nx


def fold(x):
    rows, cols = x.shape
    x = jnp.sum(x.reshape(rows // SUBLANES, SUBLANES, cols), axis=0)
    acc = x[:, 0:LANES]
    for c in range(LANES, cols, LANES):
        acc = acc + x[:, c : c + LANES]
    return acc


def greet(axes):
    barrier = pltpu.get_barrier_semaphore()
    total = 0
    for name, size in axes:
        mine = lax.axis_index(name)
        for d in range(1, size):
            peer = lax.rem(mine + d, size)
            pl.semaphore_signal(barrier, inc=1, device_id={name: peer}, device_id_type=MESH)
        total += size - 1
    pl.semaphore_wait(barrier, total)


def step_kernel(
    n, ne, nx, grid_c, entries,
    act, cots, nxt, w_hbm, m_hbm, v_hbm,
    w_out, m_out, v_out, wb_out, nxt_all,
    acts, cot_all, w, m, v, sq_src, sq_all, ex_src, ex_all, up_src, up_all,
    load_sem, own_sem,
    az_send, az_recv, ax_send, ax_recv, nz_send, nz_recv, nx_send, nx_recv,
    cot_send, cot_recv, sq_send, sq_recv, ex_send, ex_recv, up_send, up_recv,
):
    nz = n // nx
    me = lax.axis_index("shard")
    ex = lax.axis_index("expert")
    iz, ix = me // nx, lax.rem(me, nx)
    cap, d_full = act.shape
    d_blk, f_blk = w.shape
    half = cap // 2
    row0 = pl.multiple_of((me // grid_c) * d_blk, d_blk)

    loads = [
        pltpu.make_async_copy(src, dst, load_sem.at[i])
        for i, (src, dst) in enumerate(((w_hbm, w), (m_hbm, m), (v_hbm, v)))
    ]
    owns = [
        pltpu.make_async_copy(act, acts.at[me], own_sem.at[0]),
        pltpu.make_async_copy(nxt, nxt_all.at[me], own_sem.at[1]),
        pltpu.make_async_copy(cots.at[lax.rem(me, grid_c)], cot_all.at[me], own_sem.at[2]),
    ]
    for c in owns + loads:
        c.start()
    greet((("shard", n), ("expert", ne)))
    owns[0].wait()
    owns[1].wait()

    sends = []

    def send(src, dst, s, r, peer, axis="shard", when=None):
        c = pltpu.make_async_remote_copy(
            src_ref=src, dst_ref=dst, send_sem=s, recv_sem=r,
            device_id={axis: peer}, device_id_type=MESH,
        )
        if when is None:
            c.start()
        else:
            pl.when(when)(c.start)
        sends.append((when, c))

    def z_slot(k):
        return lax.rem(iz + k + nz, nz) * nx + ix

    def part(buf, slot, p):
        return buf.at[slot, pl.ds(p * half, half)]

    def holds(h, t):
        return iz >= t if h == 0 else iz < nz - t

    def z_send(buf, t, h, p, zs, zr):
        way = 1 - 2 * h
        slot = z_slot(-way * (t - 1))
        more = jnp.logical_and(iz >= t - 1, iz < nz - 1) if h == 0 else jnp.logical_and(iz <= nz - t, iz > 0)
        send(part(buf, slot, p), part(buf, slot, p), zs.at[h, p, t], zr.at[h, p, t], z_slot(way), when=more)

    def x_send(buf, t, h, p, xs, xr):
        way = 1 - 2 * h
        slot = z_slot(-way * t)
        for d in range(1, nx):
            peer = iz * nx + lax.rem(ix + d, nx)
            send(
                part(buf, slot, p), part(buf, slot, p), xs.at[h, p, t, d], xr.at[h, p, t, d], peer,
                when=None if t == 0 else holds(h, t),
            )

    def arrived(buf, slot, p, sem, when=None):
        ref = part(buf, slot, p)
        c = pltpu.make_async_copy(ref, ref, sem)
        if when is None:
            c.wait()
        else:
            pl.when(when)(c.wait)

    def own_sends(buf, zs, zr, xs, xr):
        for p in range(2):
            if nz > 1:
                for h in range(2):
                    z_send(buf, 1, h, p, zs, zr)
            x_send(buf, 0, 0, p, xs, xr)

    def relay(buf, t, zs, zr, xs, xr):
        for p in range(2):
            for h in range(2):
                arrived(buf, z_slot(-(1 - 2 * h) * t), p, zr.at[h, p, t], when=holds(h, t))
                if t < nz - 1:
                    z_send(buf, t + 1, h, p, zs, zr)
                x_send(buf, t, h, p, xs, xr)

    def finish(buf, xr):
        for t in range(nz):
            for h in range(2 if t else 1):
                for p in range(2):
                    for d in range(1, nx):
                        slot = lax.rem(iz - (1 - 2 * h) * t + nz, nz) * nx + lax.rem(ix - d + nx, nx)
                        arrived(buf, slot, p, xr.at[h, p, t, d], when=holds(h, t) if t else None)

    def cot_sends(ds):
        for d in ds:
            peer = lax.rem(me + d, n)
            send(cots.at[lax.rem(peer, grid_c)], cot_all.at[me], cot_send.at[d], cot_recv.at[d], peer)

    acts_sems = (az_send, az_recv, ax_send, ax_recv)
    nxt_sems = (nz_send, nz_recv, nx_send, nx_recv)
    own_sends(acts, *acts_sems)
    order = sorted(range(1, n), key=lambda d: -min(d, n - d))
    share = -(-len(order) // nz)
    cot_sends(order[:share])
    for t in range(1, nz):
        relay(acts, t, *acts_sems)
        cot_sends(order[share * t : share * (t + 1)])
    own_sends(nxt_all, *nxt_sems)

    tile = 64
    loads[0].wait()

    def w_body(i, acc):
        x = w[pl.ds(i * tile, tile), :]
        return acc + fold(x * x)

    zero = jnp.zeros((SUBLANES, LANES), jnp.float32)
    up_src[0] = lax.fori_loop(0, d_blk // tile, w_body, zero)
    loads[1].wait()
    loads[2].wait()
    finish(acts, ax_recv)
    owns[2].wait()
    for d in range(1, n):
        slot = lax.rem(me - d + n, n)
        pltpu.make_async_copy(cot_all.at[slot], cot_all.at[slot], cot_recv.at[d]).wait()

    g_tile = 256

    def g_body(i, acc):
        a = acts[:, :, pl.ds(pl.multiple_of(row0 + i * g_tile, g_tile), g_tile)]
        g = lax.dot_general(
            a.reshape(n * cap, g_tile), cot_all[...].reshape(n * cap, f_blk),
            (((0,), (0,)), ((), ())), preferred_element_type=jnp.float32,
        )
        w_out[pl.ds(pl.multiple_of(i * g_tile, g_tile), g_tile), :] = g
        return acc + fold(g * g)

    sq_src[...] = lax.fori_loop(0, d_blk // g_tile, g_body, zero)

    def spread(src, dst, ss, rs, axis, mine, size):
        for d in range(1, size):
            send(src, dst.at[mine], ss.at[d], rs.at[d], lax.rem(mine + d, size), axis)

    def collect(src, dst, rs, mine, size):
        total = src[...]
        for d in range(1, size):
            slot = lax.rem(mine - d + size, size)
            pltpu.make_async_copy(dst.at[slot], dst.at[slot], rs.at[d]).wait()
            total = total + dst[slot]
        return total

    spread(sq_src, sq_all, sq_send, sq_recv, "shard", me, n)
    if nz > 1:
        relay(nxt_all, 1, *nxt_sems)
    ex_src[...] = collect(sq_src, sq_all, sq_recv, me, n)
    spread(ex_src, ex_all, ex_send, ex_recv, "expert", ex, ne)
    norm_total = jnp.sum(collect(ex_src, ex_all, ex_recv, ex, ne), keepdims=True)
    rms = jnp.sqrt(norm_total / entries + 1e-06)
    clip = jnp.minimum(1.0, 1.0 / rms)
    for t in range(2, nz):
        if t < nz - 1:
            relay(nxt_all, t, *nxt_sems)

    u_tile = 32

    def u_body(i, acc):
        rows = pl.ds(pl.multiple_of(i * u_tile, u_tile), u_tile)
        g = clip * w_out[rows, :]
        m_new = 0.9 * m[rows, :].astype(jnp.float32) + 0.1 * g
        v_new = 0.999 * v[rows, :].astype(jnp.float32) + 0.001 * g * g
        m_out[rows, :] = m_new.astype(jnp.bfloat16)
        v_out[rows, :] = v_new.astype(jnp.bfloat16)
        scaled = m_new * (1.0 / (1.0 - 0.9**10))
        root = jnp.sqrt(v_new * (1.0 / (1.0 - 0.999**10)))
        u = scaled / (root + 1e-06) + 0.01 * w[rows, :]
        w_out[rows, :] = u
        return acc + fold(u * u)

    up_src[1] = lax.fori_loop(0, d_blk // u_tile, u_body, zero)
    spread(up_src, up_all, up_send, up_recv, "shard", me, n)
    if nz > 2:
        relay(nxt_all, nz - 1, *nxt_sems)
    sums = collect(up_src, up_all, up_recv, me, n)
    trust = jnp.sqrt(jnp.sum(sums[0], keepdims=True)) / (
        jnp.sqrt(jnp.sum(sums[1], keepdims=True)) + 1e-06
    )
    rate = 0.08 * trust

    def p_body(i, carry):
        rows = pl.ds(pl.multiple_of(i * u_tile, u_tile), u_tile)
        x = w[rows, :] - rate * w_out[rows, :]
        w_out[rows, :] = x
        wb_out[rows, :] = x.astype(jnp.bfloat16)
        return carry

    lax.fori_loop(0, d_blk // u_tile, p_body, 0)
    finish(nxt_all, nx_recv)
    for when, c in sends:
        if when is None:
            c.wait_send()
        else:
            pl.when(when)(c.wait_send)


def project_kernel(n, grid_c, chunks, nxt_all, wb, got, made, own_sem, send_sem, recv_sem):
    me = lax.axis_index("shard")
    d_blk, f_blk = wb.shape
    cap = nxt_all.shape[1]
    row0 = pl.multiple_of((me // grid_c) * d_blk, d_blk)
    greet((("shard", n),))
    copies = []
    start = 0
    for k, width in enumerate(chunks):
        cols = pl.ds(start, width)
        x = nxt_all[:, :, pl.ds(row0, d_blk)].reshape(n * cap, d_blk)
        y = jnp.dot(x, wb[:, cols], preferred_element_type=jnp.float32)
        made[:, :, cols] = y.astype(made.dtype).reshape(n, cap, width)
        for d in range(1, n):
            peer = lax.rem(me + d, n)
            c = pltpu.make_async_remote_copy(
                src_ref=made.at[peer, :, cols], dst_ref=got.at[me, :, cols],
                send_sem=send_sem.at[k, d], recv_sem=recv_sem.at[k, d],
                device_id={"shard": peer}, device_id_type=MESH,
            )
            c.start()
            copies.append(c)
        start += width
    own = pltpu.make_async_copy(made.at[me], got.at[me], own_sem.at[0])
    own.start()
    own.wait()
    start = 0
    for k, width in enumerate(chunks):
        for d in range(1, n):
            ref = got.at[lax.rem(me - d + n, n), :, pl.ds(start, width)]
            pltpu.make_async_copy(ref, ref, recv_sem.at[k, d]).wait()
        start += width
    for c in copies:
        c.wait_send()


def store_kernel(*refs):
    count = len(refs) // 2
    sems = refs[-1]
    copies = [pltpu.make_async_copy(refs[i], refs[count + i], sems.at[i]) for i in range(count)]
    for c in copies:
        c.start()
    for c in copies:
        c.wait()


def split_lanes(f_blk, parts):
    units = f_blk // LANES
    parts = min(parts, units)
    return tuple((units // parts + (1 if i >= parts - units % parts else 0)) * LANES for i in range(parts))


def split_body(activations, out_grads, next_inputs, counts, master, moment, second):
    n = lax.axis_size("shard")
    ne = lax.axis_size("expert")
    cap, d_full = activations.shape[2:]
    ff = out_grads.shape[3]
    d_blk, f_blk = master.shape[2:]
    grid_r, grid_c = d_full // d_blk, ff // f_blk
    nx = columns_of(n)
    nz = n // nx
    entries = float(ne * master.shape[0] * d_full * ff)
    valid = lax.iota(jnp.int32, cap) < counts[0, 0]
    masked = jnp.where(valid[:, None], out_grads[0, 0], jnp.zeros((), jnp.bfloat16))
    cots = masked.reshape(cap, grid_c, f_blk).transpose(1, 0, 2)

    f32, bf16 = jnp.float32, jnp.bfloat16
    any_spec = pl.BlockSpec(memory_space=pl.ANY)
    vmem_spec = pl.BlockSpec(memory_space=pltpu.VMEM)
    dma = pltpu.SemaphoreType.DMA
    sq = (SUBLANES, LANES)
    w_new, m_new, v_new, wb, nxt_all = pl.pallas_call(
        functools.partial(step_kernel, n, ne, nx, grid_c, entries),
        out_shape=(
            pltpu.VMEM((d_blk, f_blk), f32),
            pltpu.VMEM((d_blk, f_blk), bf16),
            pltpu.VMEM((d_blk, f_blk), bf16),
            pltpu.VMEM((d_blk, f_blk), bf16),
            pltpu.VMEM((n, cap, d_full), bf16),
        ),
        in_specs=[any_spec] * 3 + [pl.BlockSpec(memory_space=pltpu.HBM)] * 3,
        out_specs=(vmem_spec,) * 5,
        scratch_shapes=[
            pltpu.VMEM((n, cap, d_full), bf16),
            pltpu.VMEM((n, cap, f_blk), bf16),
            pltpu.VMEM((d_blk, f_blk), f32),
            pltpu.VMEM((d_blk, f_blk), bf16),
            pltpu.VMEM((d_blk, f_blk), bf16),
            pltpu.VMEM(sq, f32),
            pltpu.VMEM((n,) + sq, f32),
            pltpu.VMEM(sq, f32),
            pltpu.VMEM((ne,) + sq, f32),
            pltpu.VMEM((2,) + sq, f32),
            pltpu.VMEM((n, 2) + sq, f32),
            dma((3,)),
            dma((3,)),
        ]
        + [dma((2, 2, nz)), dma((2, 2, nz)), dma((2, 2, nz, nx)), dma((2, 2, nz, nx))] * 2
        + [dma((n,)), dma((n,)), dma((n,)), dma((n,)), dma((ne,)), dma((ne,)), dma((n,)), dma((n,))],
        compiler_params=pltpu.CompilerParams(
            collective_id=0, has_side_effects=True, vmem_limit_bytes=26 * 2**20
        ),
    )(activations[0, 0], cots, next_inputs[0, 0], master[0, 0], moment[0, 0], second[0, 0])

    w_new, m_new, v_new = pl.pallas_call(
        store_kernel,
        out_shape=tuple(jax.ShapeDtypeStruct(x.shape, x.dtype) for x in (w_new, m_new, v_new)),
        in_specs=[vmem_spec] * 3,
        out_specs=(any_spec,) * 3,
        scratch_shapes=[dma((3,))],
        compiler_params=pltpu.CompilerParams(vmem_limit_bytes=2**20),
    )(w_new, m_new, v_new)

    back = bf16 if grid_r == 1 else f32
    chunks = split_lanes(f_blk, 3)
    got = pl.pallas_call(
        functools.partial(project_kernel, n, grid_c, chunks),
        out_shape=jax.ShapeDtypeStruct((n, cap, f_blk), back),
        in_specs=[vmem_spec] * 2,
        out_specs=vmem_spec,
        scratch_shapes=[
            pltpu.VMEM((n, cap, f_blk), back),
            dma((1,)),
            dma((len(chunks), n)),
            dma((len(chunks), n)),
        ],
        compiler_params=pltpu.CompilerParams(
            collective_id=1, has_side_effects=True, vmem_limit_bytes=16 * 2**20
        ),
    )(nxt_all, wb)
    summed = jnp.sum(got.reshape(grid_r, grid_c, cap, f_blk), axis=0)
    projected = summed.transpose(1, 0, 2).reshape(cap, ff).astype(bf16)
    return w_new[None, None], m_new[None, None], v_new[None, None], projected[None, None]


def flip(z, k, top):
    out, bit = z, 1
    while bit < top:
        out = out + lax.rem(lax.div(k, bit), 2) * bit * (1 - 2 * lax.rem(lax.div(z, bit), 2))
        bit *= 2
    return out


def fused_kernel(
    n, ne, nx, entries, parts, halves, pieces,
    cnt_hbm, act, cot_hbm, nxt, w_hbm, m_hbm, v_hbm,
    w_out, m_out, v_out, got,
    acts, nxt_all, cot_all, cots, w, wb, cnt, sq_src, sq_all, up_src, up_all,
    load_sem,
    az_send, az_recv, ax_send, ax_recv, nz_send, nz_recv, nx_send, nx_recv,
    cot_sem, sq_sem, up_sem, y_sem,
):
    nz = n // nx
    me = lax.axis_index("shard")
    ex = lax.axis_index("expert")
    iz, ix = lax.div(me, nx), lax.rem(me, nx)
    cap, d_full = act.shape
    d_blk, f_blk = w.shape

    barrier = pltpu.get_barrier_semaphore()
    for de in range(ne):
        for ds in range(n):
            if de or ds:
                pl.semaphore_signal(
                    barrier, inc=1, device_id_type=MESH,
                    device_id={"expert": lax.rem(ex + de, ne), "shard": lax.rem(me + ds, n)},
                )
    loads = [
        pltpu.make_async_copy(src, dst, load_sem.at[i])
        for i, (src, dst) in enumerate((
            (cnt_hbm, cnt), (act, acts.at[me]), (cot_hbm, cots), (nxt, nxt_all.at[me]),
            (w_hbm, w), (m_hbm, m_out), (v_hbm, v_out),
        ))
    ]
    for c in loads:
        c.start()
    loads[0].wait()
    loads[1].wait()
    loads[2].wait()
    valid = lax.broadcasted_iota(jnp.int32, (cap, f_blk), 0) < cnt[...]

    def mask_body(j, carry):
        cols = pl.ds(pl.multiple_of(j * f_blk, LANES), f_blk)
        x = cots[:, cols].astype(jnp.float32)
        cots[:, cols] = jnp.where(valid, x, 0.0).astype(jnp.bfloat16)
        return carry

    lax.fori_loop(0, n, mask_body, 0)
    pl.semaphore_wait(barrier, ne * n - 1)

    drains = []

    def send(src, dst, s, r, shard, expert=None, when=None):
        device = {"shard": shard} if expert is None else {"expert": expert, "shard": shard}
        c = pltpu.make_async_remote_copy(
            src_ref=src, dst_ref=dst, send_sem=s, recv_sem=r, device_id=device, device_id_type=MESH,
        )
        if when is None:
            c.start()
        else:
            pl.when(when)(c.start)

    def await_copy(ref, sem, when=None):
        c = pltpu.make_async_copy(ref, ref, sem)
        if when is None:
            c.wait()
        else:
            pl.when(when)(c.wait)

    def z_slot(k):
        return lax.rem(iz + k + nz, nz) * nx + ix

    def cut(buf, slot, p, count):
        width = d_full // count
        return buf.at[slot, :, pl.ds(p * width, width)]

    def holds(h, t):
        return iz >= t if h == 0 else iz < nz - t

    def z_send(g, t, h, p):
        buf, count, zs, zr, _, _ = g
        way = 1 - 2 * h
        slot = z_slot(-way * (t - 1))
        more = jnp.logical_and(iz >= t - 1, iz < nz - 1) if h == 0 else jnp.logical_and(iz <= nz - t, iz > 0)
        block = cut(buf, slot, p, count)
        send(block, block, zs.at[h, t], zr.at[h, p, t], z_slot(way), when=more)
        if p == 0:
            drains.append((buf.at[slot], zs.at[h, t], more))

    def x_send(g, t, h, p):
        buf, count, _, _, xs, xr = g
        slot = z_slot(-(1 - 2 * h) * t)
        when = None if t == 0 else holds(h, t)
        block = cut(buf, slot, p, count)
        for d in range(1, nx):
            landing = xr.at[p] if buf is acts else xr.at[h, t, d - 1]
            send(block, block, xs.at[h, t, d - 1], landing, iz * nx + lax.rem(ix + d, nx), when=when)
            if p == 0:
                drains.append((buf.at[slot], xs.at[h, t, d - 1], when))

    def own_z(g, p):
        if nz > 1:
            for h in range(2):
                z_send(g, 1, h, p)

    def own(g, ps):
        for p in ps:
            own_z(g, p)
            x_send(g, 0, 0, p)

    def relay(g, t, ps):
        for p in ps:
            for h in range(2):
                await_copy(cut(g[0], z_slot(-(1 - 2 * h) * t), p, g[1]), g[3].at[h, p, t], holds(h, t))
                if t < nz - 1:
                    z_send(g, t + 1, h, p)
                x_send(g, t, h, p)

    def peer_to(k, dx):
        return flip(iz, k, nz) * nx + lax.rem(ix + dx, nx)

    def cot_sends(which):
        for k, dx in which:
            peer = peer_to(k, dx)
            cols = pl.ds(pl.multiple_of(peer * f_blk, LANES), f_blk)
            send(cots.at[:, cols], cot_all.at[me], cot_sem.at[0], cot_sem.at[1], peer)

    g_acts = (acts, parts, az_send, az_recv, ax_send, ax_recv)
    g_nxt = (nxt_all, halves, nz_send, nz_recv, nx_send, nx_recv)
    every, each = range(parts), range(halves)
    tile = 64

    def w_body(i, acc):
        x = w[pl.ds(pl.multiple_of(i * tile, tile), tile), :]
        return acc + fold(x * x)

    zero = jnp.zeros((SUBLANES, LANES), jnp.float32)
    far = sorted(range(1, nz), key=lambda k: (-k.bit_length(), k))
    near = [(0, dx) for dx in range(1, nx)]
    order = near + [(k, 0) for k in far] + [(k, dx) for k in far for dx in range(1, nx)]
    share = -(-len(order) // max(nz - 1, 1))
    cuts = [share * (t + 1) for t in range(nz)]

    own(g_acts, every)
    cot_sends(order[: cuts[0]])
    cot_all[me] = cots[:, pl.ds(pl.multiple_of(me * f_blk, LANES), f_blk)]
    squares = zero
    for t in range(1, nz):
        relay(g_acts, t, every)
        cot_sends(order[cuts[t - 1] : cuts[t]])
        if t == 1:
            loads[4].wait()
            squares = lax.fori_loop(0, d_blk // tile, w_body, zero)
    up_src[0:1] = jnp.sum(squares, axis=0, keepdims=True)
    await_copy(cot_all.at[pl.ds(0, n - 1)], cot_sem.at[1])

    g_tile = 256
    total = zero
    per = d_full // parts // g_tile

    def g_body(i, acc):
        rows = pl.ds(pl.multiple_of(i * g_tile, g_tile), g_tile)
        g = lax.dot_general(
            acts[:, :, rows].reshape(n * cap, g_tile), cot_all[...].reshape(n * cap, f_blk),
            (((0,), (0,)), ((), ())), preferred_element_type=jnp.float32,
        )
        w_out[rows, :] = g
        return acc + fold(g * g)

    for p in every:
        if nx > 1:
            width = d_full // parts
            await_copy(acts.at[pl.ds(0, nz * (nx - 1)), :, pl.ds(p * width, width)], ax_recv.at[p])
        total = lax.fori_loop(p * per, (p + 1) * per, g_body, total)
    sq_src[...] = jnp.sum(total, axis=0, keepdims=True)
    for de in range(ne):
        for ds in range(n):
            if de or ds:
                send(
                    sq_src, sq_all.at[de * n + ds], sq_sem.at[0], sq_sem.at[1],
                    lax.rem(me + ds, n), lax.rem(ex + de, ne),
                )
    loads[3].wait()
    own(g_nxt, each)
    loads[5].wait()
    loads[6].wait()
    await_copy(sq_all.at[pl.ds(1, ne * n - 1)], sq_sem.at[1])
    norm = sq_src[...]
    for k in range(1, ne * n):
        norm = norm + sq_all[k]
    rms = jnp.sqrt(jnp.sum(norm, keepdims=True) / entries + 1e-06)
    clip = jnp.minimum(1.0, 1.0 / rms)

    u_tile = 32
    first_scale, later_scale = 1.0 / (1.0 - 0.9**10), 1.0 / (1.0 - 0.999**10)

    def u_body(i, acc):
        rows = pl.ds(pl.multiple_of(i * u_tile, u_tile), u_tile)
        g = clip * w_out[rows, :]
        m_new = 0.9 * m_out[rows, :].astype(jnp.float32) + 0.1 * g
        v_new = 0.999 * v_out[rows, :].astype(jnp.float32) + 0.001 * g * g
        m_out[rows, :] = m_new.astype(jnp.bfloat16)
        v_out[rows, :] = v_new.astype(jnp.bfloat16)
        later = v_new * later_scale
        root = later * lax.rsqrt(later)
        u = (m_new * first_scale) / (root + 1e-06) + 0.01 * w[rows, :]
        w_out[rows, :] = u
        return acc + fold(u * u)

    def u_span(first, last, acc):
        return lax.fori_loop(first, last, u_body, acc)

    steps = d_blk // u_tile
    early = 1
    mid = steps * 3 // 4
    acc = u_span(0, mid, zero)
    if nz > 1:
        relay(g_nxt, 1, each[:early])
    acc = u_span(mid, steps, acc)
    up_src[1:2] = jnp.sum(acc, axis=0, keepdims=True)
    for ds in range(1, n):
        send(up_src, up_all.at[ds], up_sem.at[0], up_sem.at[1], lax.rem(me + ds, n))
    if nz > 1:
        relay(g_nxt, 1, each[early:])
    await_copy(up_all.at[pl.ds(1, n - 1)], up_sem.at[1])
    sums = up_src[...]
    for ds in range(1, n):
        sums = sums + up_all[ds]
    trust = jnp.sqrt(jnp.sum(sums[0:1], keepdims=True)) / (jnp.sqrt(jnp.sum(sums[1:2], keepdims=True)) + 1e-06)
    rate = 0.08 * trust

    def p_body(i, carry):
        rows = pl.ds(pl.multiple_of(i * u_tile, u_tile), u_tile)
        x = w[rows, :] - rate * w_out[rows, :]
        w_out[rows, :] = x
        wb[rows, :] = x.astype(jnp.bfloat16)
        return carry

    lax.fori_loop(0, steps, p_body, 0)

    def crossed(t):
        for h in range(2 if t else 1):
            for d in range(1, nx):
                slot = lax.rem(iz - (1 - 2 * h) * t + nz, nz) * nx + lax.rem(ix - d + nx, nx)
                await_copy(nxt_all.at[slot], nx_recv.at[h, t, d - 1], holds(h, t) if t else None)

    def project(k, dx):
        peer = peer_to(k, dx)
        start = 0
        for piece in pieces:
            cols = pl.ds(start, piece)
            y = jnp.dot(nxt_all[peer], wb[:, cols], preferred_element_type=jnp.float32)
            cot_all[peer, :, cols] = y.astype(jnp.bfloat16)
            if dx or not (isinstance(k, int) and k == 0):
                mine = pl.ds(pl.multiple_of(me * f_blk + start, LANES), piece)
                send(cot_all.at[peer, :, cols], got.at[:, mine], y_sem.at[0], y_sem.at[1], peer)
            start += piece

    if nz == 4:
        inner = lax.rem(lax.div(iz + 1, 2), 2)
        ks = [1 + 2 * inner, 2, 3 - 2 * inner]
    else:
        ks = far
    others = range(1, nx)
    if nz == 4:
        project(ks[0], 0)
        relay(g_nxt, 2, each)
        project(ks[1], 0)
        crossed(0)
        crossed(1)
        for dx in others:
            project(ks[0], dx)
        relay(g_nxt, 3, each)
        project(ks[2], 0)
        crossed(2)
        for dx in others:
            project(ks[1], dx)
        crossed(3)
        for dx in others:
            project(ks[2], dx)
    else:
        for t in range(2, nz):
            relay(g_nxt, t, each)
        for t in range(nz):
            crossed(t)
        for k in ks:
            for dx in range(nx):
                project(k, dx)
    for dx in others:
        project(0, dx)
    project(0, 0)
    got[:, pl.ds(pl.multiple_of(me * f_blk, LANES), f_blk)] = cot_all[me]
    if n > 1:
        await_copy(got.at[:, pl.ds(0, (n - 1) * f_blk)], y_sem.at[1])
        drains.append((got.at[:, pl.ds(0, (n - 1) * f_blk)], y_sem.at[0], None))
        drains.append((cot_all.at[pl.ds(0, n - 1)], cot_sem.at[0], None))
        drains.append((up_all.at[pl.ds(1, n - 1)], up_sem.at[0], None))
    drains.append((sq_all.at[pl.ds(1, ne * n - 1)], sq_sem.at[0], None))
    for ref, sem, when in drains:
        await_copy(ref, sem, when)


def fused_body(activations, out_grads, next_inputs, counts, master, moment, second):
    n = lax.axis_size("shard")
    ne = lax.axis_size("expert")
    cap, d_full = activations.shape[2:]
    ff = out_grads.shape[3]
    d_blk, f_blk = master.shape[2:]
    nx = columns_of(n)
    nz = n // nx
    entries = float(ne * master.shape[0] * d_full * ff)
    f32, bf16 = jnp.float32, jnp.bfloat16
    any_spec = pl.BlockSpec(memory_space=pl.ANY)
    vmem_spec = pl.BlockSpec(memory_space=pltpu.VMEM)
    dma = pltpu.SemaphoreType.DMA
    parts = 4
    pieces = split_lanes(f_blk, 2)
    halves = 2
    across = dma((2, nz, max(nx - 1, 1)))
    results = pl.pallas_call(
        functools.partial(fused_kernel, n, ne, nx, entries, parts, halves, pieces),
        out_shape=(
            pltpu.VMEM((d_blk, f_blk), f32),
            pltpu.VMEM((d_blk, f_blk), bf16),
            pltpu.VMEM((d_blk, f_blk), bf16),
            pltpu.VMEM((cap, ff), bf16),
        ),
        in_specs=[pl.BlockSpec(memory_space=pltpu.HBM)] * 7,
        out_specs=(vmem_spec,) * 4,
        scratch_shapes=[
            pltpu.VMEM((n, cap, d_full), bf16),
            pltpu.VMEM((n, cap, d_full), bf16),
            pltpu.VMEM((n, cap, f_blk), bf16),
            pltpu.VMEM((cap, ff), bf16),
            pltpu.VMEM((d_blk, f_blk), f32),
            pltpu.VMEM((d_blk, f_blk), bf16),
            pltpu.VMEM((1, 1), jnp.int32),
            pltpu.VMEM((1, LANES), f32),
            pltpu.VMEM((ne * n, 1, LANES), f32),
            pltpu.VMEM((2, LANES), f32),
            pltpu.VMEM((n, 2, LANES), f32),
            dma((7,)),
        ]
        + [dma((2, nz)), dma((2, parts, nz)), across, dma((parts,))]
        + [dma((2, nz)), dma((2, halves, nz)), across, across]
        + [dma((2,))] * 4,
        compiler_params=pltpu.CompilerParams(
            collective_id=0, has_side_effects=True, vmem_limit_bytes=47 * 2**20
        ),
    )(counts, activations[0, 0], out_grads[0, 0], next_inputs[0, 0], master[0, 0], moment[0, 0], second[0, 0])
    outs = pl.pallas_call(
        store_kernel,
        out_shape=tuple(jax.ShapeDtypeStruct(x.shape, x.dtype) for x in results),
        in_specs=[vmem_spec] * 4,
        out_specs=(any_spec,) * 4,
        scratch_shapes=[dma((4,))],
        compiler_params=pltpu.CompilerParams(vmem_limit_bytes=2**20),
    )(*results)
    return tuple(x[None, None] for x in outs)


def body(activations, out_grads, next_inputs, counts, master, moment, second):
    n = lax.axis_size("shard")
    nz = n // columns_of(n)
    whole_rows = activations.shape[3] == master.shape[2]
    step = fused_body if whole_rows and nz & (nz - 1) == 0 else split_body
    return step(activations, out_grads, next_inputs, counts, master, moment, second)


def solution(mesh):
    spec = P("expert", "shard", None, None)
    return jax.shard_map(
        body,
        mesh=mesh,
        in_specs=(spec, spec, spec, P("expert", "shard"), spec, spec, spec),
        out_specs=(spec,) * 4,
        check_vma=False,
    )
```

```python
import functools
import jax
import jax.numpy as jnp
from jax import lax
from jax.experimental import pallas as pl
from jax.experimental.pallas import tpu as pltpu
from jax.sharding import PartitionSpec as P

MESH = pl.DeviceIdType.MESH
LANES = 128
SUBLANES = 8


def columns_of(n):
    nx = 1
    while n % (2 * nx) == 0 and 8 * nx * nx <= n:
        nx *= 2
    return nx


def fold(x):
    rows, cols = x.shape
    x = jnp.sum(x.reshape(rows // SUBLANES, SUBLANES, cols), axis=0)
    acc = x[:, 0:LANES]
    for c in range(LANES, cols, LANES):
        acc = acc + x[:, c : c + LANES]
    return acc


def greet(axes):
    barrier = pltpu.get_barrier_semaphore()
    total = 0
    for name, size in axes:
        mine = lax.axis_index(name)
        for d in range(1, size):
            peer = lax.rem(mine + d, size)
            pl.semaphore_signal(barrier, inc=1, device_id={name: peer}, device_id_type=MESH)
        total += size - 1
    pl.semaphore_wait(barrier, total)


def step_kernel(
    n, ne, nx, grid_c, entries,
    act, cots, nxt, w_hbm, m_hbm, v_hbm,
    w_out, m_out, v_out, wb_out, nxt_all,
    acts, cot_all, w, m, v, sq_src, sq_all, ex_src, ex_all, up_src, up_all,
    load_sem, own_sem,
    az_send, az_recv, ax_send, ax_recv, nz_send, nz_recv, nx_send, nx_recv,
    cot_send, cot_recv, sq_send, sq_recv, ex_send, ex_recv, up_send, up_recv,
):
    nz = n // nx
    me = lax.axis_index("shard")
    ex = lax.axis_index("expert")
    iz, ix = me // nx, lax.rem(me, nx)
    cap, d_full = act.shape
    d_blk, f_blk = w.shape
    half = cap // 2
    row0 = pl.multiple_of((me // grid_c) * d_blk, d_blk)

    loads = [
        pltpu.make_async_copy(src, dst, load_sem.at[i])
        for i, (src, dst) in enumerate(((w_hbm, w), (m_hbm, m), (v_hbm, v)))
    ]
    owns = [
        pltpu.make_async_copy(act, acts.at[me], own_sem.at[0]),
        pltpu.make_async_copy(nxt, nxt_all.at[me], own_sem.at[1]),
        pltpu.make_async_copy(cots.at[lax.rem(me, grid_c)], cot_all.at[me], own_sem.at[2]),
    ]
    for c in owns + loads:
        c.start()
    greet((("shard", n), ("expert", ne)))
    owns[0].wait()
    owns[1].wait()

    sends = []

    def send(src, dst, s, r, peer, axis="shard", when=None):
        c = pltpu.make_async_remote_copy(
            src_ref=src, dst_ref=dst, send_sem=s, recv_sem=r,
            device_id={axis: peer}, device_id_type=MESH,
        )
        if when is None:
            c.start()
        else:
            pl.when(when)(c.start)
        sends.append((when, c))

    def z_slot(k):
        return lax.rem(iz + k + nz, nz) * nx + ix

    def part(buf, slot, p):
        return buf.at[slot, pl.ds(p * half, half)]

    def holds(h, t):
        return iz >= t if h == 0 else iz < nz - t

    def z_send(buf, t, h, p, zs, zr):
        way = 1 - 2 * h
        slot = z_slot(-way * (t - 1))
        more = jnp.logical_and(iz >= t - 1, iz < nz - 1) if h == 0 else jnp.logical_and(iz <= nz - t, iz > 0)
        send(part(buf, slot, p), part(buf, slot, p), zs.at[h, p, t], zr.at[h, p, t], z_slot(way), when=more)

    def x_send(buf, t, h, p, xs, xr):
        way = 1 - 2 * h
        slot = z_slot(-way * t)
        for d in range(1, nx):
            peer = iz * nx + lax.rem(ix + d, nx)
            send(
                part(buf, slot, p), part(buf, slot, p), xs.at[h, p, t, d], xr.at[h, p, t, d], peer,
                when=None if t == 0 else holds(h, t),
            )

    def arrived(buf, slot, p, sem, when=None):
        ref = part(buf, slot, p)
        c = pltpu.make_async_copy(ref, ref, sem)
        if when is None:
            c.wait()
        else:
            pl.when(when)(c.wait)

    def own_sends(buf, zs, zr, xs, xr):
        for p in range(2):
            if nz > 1:
                for h in range(2):
                    z_send(buf, 1, h, p, zs, zr)
            x_send(buf, 0, 0, p, xs, xr)

    def relay(buf, t, zs, zr, xs, xr):
        for p in range(2):
            for h in range(2):
                arrived(buf, z_slot(-(1 - 2 * h) * t), p, zr.at[h, p, t], when=holds(h, t))
                if t < nz - 1:
                    z_send(buf, t + 1, h, p, zs, zr)
                x_send(buf, t, h, p, xs, xr)

    def finish(buf, xr):
        for t in range(nz):
            for h in range(2 if t else 1):
                for p in range(2):
                    for d in range(1, nx):
                        slot = lax.rem(iz - (1 - 2 * h) * t + nz, nz) * nx + lax.rem(ix - d + nx, nx)
                        arrived(buf, slot, p, xr.at[h, p, t, d], when=holds(h, t) if t else None)

    def cot_sends(ds):
        for d in ds:
            peer = lax.rem(me + d, n)
            send(cots.at[lax.rem(peer, grid_c)], cot_all.at[me], cot_send.at[d], cot_recv.at[d], peer)

    acts_sems = (az_send, az_recv, ax_send, ax_recv)
    nxt_sems = (nz_send, nz_recv, nx_send, nx_recv)
    own_sends(acts, *acts_sems)
    order = sorted(range(1, n), key=lambda d: -min(d, n - d))
    share = -(-len(order) // nz)
    cot_sends(order[:share])
    for t in range(1, nz):
        relay(acts, t, *acts_sems)
        cot_sends(order[share * t : share * (t + 1)])
    own_sends(nxt_all, *nxt_sems)

    tile = 64
    loads[0].wait()

    def w_body(i, acc):
        x = w[pl.ds(i * tile, tile), :]
        return acc + fold(x * x)

    zero = jnp.zeros((SUBLANES, LANES), jnp.float32)
    up_src[0] = lax.fori_loop(0, d_blk // tile, w_body, zero)
    loads[1].wait()
    loads[2].wait()
    finish(acts, ax_recv)
    owns[2].wait()
    for d in range(1, n):
        slot = lax.rem(me - d + n, n)
        pltpu.make_async_copy(cot_all.at[slot], cot_all.at[slot], cot_recv.at[d]).wait()

    g_tile = 256

    def g_body(i, acc):
        a = acts[:, :, pl.ds(pl.multiple_of(row0 + i * g_tile, g_tile), g_tile)]
        g = lax.dot_general(
            a.reshape(n * cap, g_tile), cot_all[...].reshape(n * cap, f_blk),
            (((0,), (0,)), ((), ())), preferred_element_type=jnp.float32,
        )
        w_out[pl.ds(pl.multiple_of(i * g_tile, g_tile), g_tile), :] = g
        return acc + fold(g * g)

    sq_src[...] = lax.fori_loop(0, d_blk // g_tile, g_body, zero)

    def spread(src, dst, ss, rs, axis, mine, size):
        for d in range(1, size):
            send(src, dst.at[mine], ss.at[d], rs.at[d], lax.rem(mine + d, size), axis)

    def collect(src, dst, rs, mine, size):
        total = src[...]
        for d in range(1, size):
            slot = lax.rem(mine - d + size, size)
            pltpu.make_async_copy(dst.at[slot], dst.at[slot], rs.at[d]).wait()
            total = total + dst[slot]
        return total

    spread(sq_src, sq_all, sq_send, sq_recv, "shard", me, n)
    if nz > 1:
        relay(nxt_all, 1, *nxt_sems)
    ex_src[...] = collect(sq_src, sq_all, sq_recv, me, n)
    spread(ex_src, ex_all, ex_send, ex_recv, "expert", ex, ne)
    norm_total = jnp.sum(collect(ex_src, ex_all, ex_recv, ex, ne), keepdims=True)
    rms = jnp.sqrt(norm_total / entries + 1e-06)
    clip = jnp.minimum(1.0, 1.0 / rms)
    for t in range(2, nz):
        if t < nz - 1:
            relay(nxt_all, t, *nxt_sems)

    u_tile = 32

    def u_body(i, acc):
        rows = pl.ds(pl.multiple_of(i * u_tile, u_tile), u_tile)
        g = clip * w_out[rows, :]
        m_new = 0.9 * m[rows, :].astype(jnp.float32) + 0.1 * g
        v_new = 0.999 * v[rows, :].astype(jnp.float32) + 0.001 * g * g
        m_out[rows, :] = m_new.astype(jnp.bfloat16)
        v_out[rows, :] = v_new.astype(jnp.bfloat16)
        scaled = m_new * (1.0 / (1.0 - 0.9**10))
        root = jnp.sqrt(v_new * (1.0 / (1.0 - 0.999**10)))
        u = scaled / (root + 1e-06) + 0.01 * w[rows, :]
        w_out[rows, :] = u
        return acc + fold(u * u)

    up_src[1] = lax.fori_loop(0, d_blk // u_tile, u_body, zero)
    spread(up_src, up_all, up_send, up_recv, "shard", me, n)
    if nz > 2:
        relay(nxt_all, nz - 1, *nxt_sems)
    sums = collect(up_src, up_all, up_recv, me, n)
    trust = jnp.sqrt(jnp.sum(sums[0], keepdims=True)) / (
        jnp.sqrt(jnp.sum(sums[1], keepdims=True)) + 1e-06
    )
    rate = 0.08 * trust

    def p_body(i, carry):
        rows = pl.ds(pl.multiple_of(i * u_tile, u_tile), u_tile)
        x = w[rows, :] - rate * w_out[rows, :]
        w_out[rows, :] = x
        wb_out[rows, :] = x.astype(jnp.bfloat16)
        return carry

    lax.fori_loop(0, d_blk // u_tile, p_body, 0)
    finish(nxt_all, nx_recv)
    for when, c in sends:
        if when is None:
            c.wait_send()
        else:
            pl.when(when)(c.wait_send)


def project_kernel(n, grid_c, chunks, nxt_all, wb, got, made, own_sem, send_sem, recv_sem):
    me = lax.axis_index("shard")
    d_blk, f_blk = wb.shape
    cap = nxt_all.shape[1]
    row0 = pl.multiple_of((me // grid_c) * d_blk, d_blk)
    greet((("shard", n),))
    copies = []
    start = 0
    for k, width in enumerate(chunks):
        cols = pl.ds(start, width)
        x = nxt_all[:, :, pl.ds(row0, d_blk)].reshape(n * cap, d_blk)
        y = jnp.dot(x, wb[:, cols], preferred_element_type=jnp.float32)
        made[:, :, cols] = y.astype(made.dtype).reshape(n, cap, width)
        for d in range(1, n):
            peer = lax.rem(me + d, n)
            c = pltpu.make_async_remote_copy(
                src_ref=made.at[peer, :, cols], dst_ref=got.at[me, :, cols],
                send_sem=send_sem.at[k, d], recv_sem=recv_sem.at[k, d],
                device_id={"shard": peer}, device_id_type=MESH,
            )
            c.start()
            copies.append(c)
        start += width
    own = pltpu.make_async_copy(made.at[me], got.at[me], own_sem.at[0])
    own.start()
    own.wait()
    start = 0
    for k, width in enumerate(chunks):
        for d in range(1, n):
            ref = got.at[lax.rem(me - d + n, n), :, pl.ds(start, width)]
            pltpu.make_async_copy(ref, ref, recv_sem.at[k, d]).wait()
        start += width
    for c in copies:
        c.wait_send()


def store_kernel(*refs):
    count = len(refs) // 2
    sems = refs[-1]
    copies = [pltpu.make_async_copy(refs[i], refs[count + i], sems.at[i]) for i in range(count)]
    for c in copies:
        c.start()
    for c in copies:
        c.wait()


def split_lanes(f_blk, parts):
    units = f_blk // LANES
    parts = min(parts, units)
    return tuple((units // parts + (1 if i >= parts - units % parts else 0)) * LANES for i in range(parts))


def split_body(activations, out_grads, next_inputs, counts, master, moment, second):
    n = lax.axis_size("shard")
    ne = lax.axis_size("expert")
    cap, d_full = activations.shape[2:]
    ff = out_grads.shape[3]
    d_blk, f_blk = master.shape[2:]
    grid_r, grid_c = d_full // d_blk, ff // f_blk
    nx = columns_of(n)
    nz = n // nx
    entries = float(ne * master.shape[0] * d_full * ff)
    valid = lax.iota(jnp.int32, cap) < counts[0, 0]
    masked = jnp.where(valid[:, None], out_grads[0, 0], jnp.zeros((), jnp.bfloat16))
    cots = masked.reshape(cap, grid_c, f_blk).transpose(1, 0, 2)

    f32, bf16 = jnp.float32, jnp.bfloat16
    any_spec = pl.BlockSpec(memory_space=pl.ANY)
    vmem_spec = pl.BlockSpec(memory_space=pltpu.VMEM)
    dma = pltpu.SemaphoreType.DMA
    sq = (SUBLANES, LANES)
    w_new, m_new, v_new, wb, nxt_all = pl.pallas_call(
        functools.partial(step_kernel, n, ne, nx, grid_c, entries),
        out_shape=(
            pltpu.VMEM((d_blk, f_blk), f32),
            pltpu.VMEM((d_blk, f_blk), bf16),
            pltpu.VMEM((d_blk, f_blk), bf16),
            pltpu.VMEM((d_blk, f_blk), bf16),
            pltpu.VMEM((n, cap, d_full), bf16),
        ),
        in_specs=[any_spec] * 3 + [pl.BlockSpec(memory_space=pltpu.HBM)] * 3,
        out_specs=(vmem_spec,) * 5,
        scratch_shapes=[
            pltpu.VMEM((n, cap, d_full), bf16),
            pltpu.VMEM((n, cap, f_blk), bf16),
            pltpu.VMEM((d_blk, f_blk), f32),
            pltpu.VMEM((d_blk, f_blk), bf16),
            pltpu.VMEM((d_blk, f_blk), bf16),
            pltpu.VMEM(sq, f32),
            pltpu.VMEM((n,) + sq, f32),
            pltpu.VMEM(sq, f32),
            pltpu.VMEM((ne,) + sq, f32),
            pltpu.VMEM((2,) + sq, f32),
            pltpu.VMEM((n, 2) + sq, f32),
            dma((3,)),
            dma((3,)),
        ]
        + [dma((2, 2, nz)), dma((2, 2, nz)), dma((2, 2, nz, nx)), dma((2, 2, nz, nx))] * 2
        + [dma((n,)), dma((n,)), dma((n,)), dma((n,)), dma((ne,)), dma((ne,)), dma((n,)), dma((n,))],
        compiler_params=pltpu.CompilerParams(
            collective_id=0, has_side_effects=True, vmem_limit_bytes=26 * 2**20
        ),
    )(activations[0, 0], cots, next_inputs[0, 0], master[0, 0], moment[0, 0], second[0, 0])

    w_new, m_new, v_new = pl.pallas_call(
        store_kernel,
        out_shape=tuple(jax.ShapeDtypeStruct(x.shape, x.dtype) for x in (w_new, m_new, v_new)),
        in_specs=[vmem_spec] * 3,
        out_specs=(any_spec,) * 3,
        scratch_shapes=[dma((3,))],
        compiler_params=pltpu.CompilerParams(vmem_limit_bytes=2**20),
    )(w_new, m_new, v_new)

    back = bf16 if grid_r == 1 else f32
    chunks = split_lanes(f_blk, 3)
    got = pl.pallas_call(
        functools.partial(project_kernel, n, grid_c, chunks),
        out_shape=jax.ShapeDtypeStruct((n, cap, f_blk), back),
        in_specs=[vmem_spec] * 2,
        out_specs=vmem_spec,
        scratch_shapes=[
            pltpu.VMEM((n, cap, f_blk), back),
            dma((1,)),
            dma((len(chunks), n)),
            dma((len(chunks), n)),
        ],
        compiler_params=pltpu.CompilerParams(
            collective_id=1, has_side_effects=True, vmem_limit_bytes=16 * 2**20
        ),
    )(nxt_all, wb)
    summed = jnp.sum(got.reshape(grid_r, grid_c, cap, f_blk), axis=0)
    projected = summed.transpose(1, 0, 2).reshape(cap, ff).astype(bf16)
    return w_new[None, None], m_new[None, None], v_new[None, None], projected[None, None]


def flip(z, k, top):
    out, bit = z, 1
    while bit < top:
        out = out + lax.rem(lax.div(k, bit), 2) * bit * (1 - 2 * lax.rem(lax.div(z, bit), 2))
        bit *= 2
    return out


def fused_kernel(
    n, ne, nx, entries, parts, strips, pieces,
    cnt_hbm, act, cot_hbm, nxt, w_hbm, m_hbm, v_hbm,
    w_out, m_out, v_out, got,
    acts, nxt_all, cot_all, cots, w, wb, cnt, sq_src, sq_all, up_src, up_all,
    load_sem,
    az_send, az_recv, ax_send, ax_recv, nz_send, nz_recv, nx_send, nx_recv,
    cot_sem, sq_sem, up_sem, y_sem,
):
    nz = n // nx
    me = lax.axis_index("shard")
    ex = lax.axis_index("expert")
    iz, ix = lax.div(me, nx), lax.rem(me, nx)
    cap, d_full = act.shape
    d_blk, f_blk = w.shape

    barrier = pltpu.get_barrier_semaphore()
    for de in range(ne):
        for ds in range(n):
            if de or ds:
                pl.semaphore_signal(
                    barrier, inc=1, device_id_type=MESH,
                    device_id={"expert": lax.rem(ex + de, ne), "shard": lax.rem(me + ds, n)},
                )
    loads = [
        pltpu.make_async_copy(src, dst, load_sem.at[i])
        for i, (src, dst) in enumerate((
            (cnt_hbm, cnt), (act, acts.at[me]), (cot_hbm, cots), (nxt, nxt_all.at[me]),
            (w_hbm, w), (m_hbm, m_out), (v_hbm, v_out),
        ))
    ]
    for c in loads:
        c.start()
    loads[0].wait()
    loads[1].wait()
    loads[2].wait()
    valid = lax.broadcasted_iota(jnp.int32, (cap, f_blk), 0) < cnt[...]

    def mask_body(j, carry):
        cols = pl.ds(pl.multiple_of(j * f_blk, LANES), f_blk)
        x = cots[:, cols].astype(jnp.float32)
        cots[:, cols] = jnp.where(valid, x, 0.0).astype(jnp.bfloat16)
        return carry

    lax.fori_loop(0, n, mask_body, 0)
    pl.semaphore_wait(barrier, ne * n - 1)

    drains = []

    def send(src, dst, s, r, shard, expert=None, when=None):
        device = {"shard": shard} if expert is None else {"expert": expert, "shard": shard}
        c = pltpu.make_async_remote_copy(
            src_ref=src, dst_ref=dst, send_sem=s, recv_sem=r, device_id=device, device_id_type=MESH,
        )
        if when is None:
            c.start()
        else:
            pl.when(when)(c.start)

    def await_copy(ref, sem, when=None):
        c = pltpu.make_async_copy(ref, ref, sem)
        if when is None:
            c.wait()
        else:
            pl.when(when)(c.wait)

    def z_slot(k):
        return lax.rem(iz + k + nz, nz) * nx + ix

    def cut(buf, slot, p):
        width = d_full // parts
        return buf.at[slot, :, pl.ds(p * width, width)]

    def holds(h, t):
        return iz >= t if h == 0 else iz < nz - t

    def z_send(g, t, h, p):
        buf, zs, zr, _, _ = g
        way = 1 - 2 * h
        slot = z_slot(-way * (t - 1))
        more = jnp.logical_and(iz >= t - 1, iz < nz - 1) if h == 0 else jnp.logical_and(iz <= nz - t, iz > 0)
        block = cut(buf, slot, p)
        send(block, block, zs.at[h, t], zr.at[h, p, t], z_slot(way), when=more)
        if p == 0:
            drains.append((buf.at[slot], zs.at[h, t], more))

    def x_send(g, t, h, p):
        buf, _, _, xs, xr = g
        slot = z_slot(-(1 - 2 * h) * t)
        when = None if t == 0 else holds(h, t)
        block = cut(buf, slot, p)
        for d in range(1, nx):
            landing = xr.at[0] if buf is acts else xr.at[h, t, d - 1]
            send(block, block, xs.at[h, t, d - 1], landing, iz * nx + lax.rem(ix + d, nx), when=when)
            if p == 0:
                drains.append((buf.at[slot], xs.at[h, t, d - 1], when))

    def own(g, ps):
        for p in ps:
            if nz > 1:
                for h in range(2):
                    z_send(g, 1, h, p)
            x_send(g, 0, 0, p)

    def relay(g, t, ps):
        for p in ps:
            for h in range(2):
                await_copy(cut(g[0], z_slot(-(1 - 2 * h) * t), p), g[2].at[h, p, t], holds(h, t))
                if t < nz - 1:
                    z_send(g, t + 1, h, p)
                x_send(g, t, h, p)

    def peer_to(k, dx):
        return flip(iz, k, nz) * nx + lax.rem(ix + dx, nx)

    def cot_send(k, dx, q):
        peer = peer_to(k, dx)
        start, span = sum(strips[:q]), strips[q]
        cols = pl.ds(pl.multiple_of(peer * f_blk + start, LANES), span)
        send(cots.at[:, cols], cot_all.at[me, :, pl.ds(start, span)], cot_sem.at[0], cot_sem.at[1 + q], peer)

    g_acts = (acts, az_send, az_recv, ax_send, ax_recv)
    g_nxt = (nxt_all, nz_send, nz_recv, nx_send, nx_recv)
    every = range(parts)
    tile = 64

    def w_body(i, acc):
        x = w[pl.ds(pl.multiple_of(i * tile, tile), tile), :]
        return acc + fold(x * x)

    zero = jnp.zeros((SUBLANES, LANES), jnp.float32)
    if nz == 4:
        inner = lax.rem(lax.div(iz + 1, 2), 2)
        ks = [1 + 2 * inner, 2, 3 - 2 * inner]
    else:
        ks = sorted(range(1, nz), key=lambda k: (-k.bit_length(), k))
    others = range(1, nx)

    def exchange(k, q):
        for dx in range(nx):
            cot_send(k, dx, q)

    def near(q):
        for dx in others:
            cot_send(0, dx, q)

    own(g_acts, every)
    if nz > 1:
        relay(g_acts, 1, every)
        exchange(ks[0], 0)
    cot_all[me] = cots[:, pl.ds(pl.multiple_of(me * f_blk, LANES), f_blk)]
    loads[4].wait()
    squares = lax.fori_loop(0, d_blk // tile, w_body, zero)
    for t in range(2, nz - 1):
        relay(g_acts, t, every)
    for k in ks[1:]:
        exchange(k, 0)
    near(0)
    if nz > 2:
        relay(g_acts, nz - 1, every)
    for q in range(1, len(strips)):
        for k in ks:
            exchange(k, q)
        near(q)
    loads[3].wait()
    own(g_nxt, every[:2])
    up_src[0:1] = jnp.sum(squares, axis=0, keepdims=True)

    g_tile = min(512, d_blk)

    if nx > 1:
        await_copy(acts.at[pl.ds(0, nz * (nx - 1))], ax_recv.at[0])
    total = zero
    for q, span in enumerate(strips):
        cols = pl.ds(sum(strips[:q]), span)
        await_copy(cot_all.at[pl.ds(0, n - 1), :, cols], cot_sem.at[1 + q])

        def g_body(i, acc):
            rows = pl.ds(pl.multiple_of(i * g_tile, g_tile), g_tile)
            g = lax.dot_general(
                acts[:, :, rows].reshape(n * cap, g_tile), cot_all[:, :, cols].reshape(n * cap, span),
                (((0,), (0,)), ((), ())), preferred_element_type=jnp.float32,
            )
            w_out[rows, cols] = g
            return acc + fold(g * g)

        total = lax.fori_loop(0, d_blk // g_tile, g_body, total)
    sq_src[...] = jnp.sum(total, axis=0, keepdims=True)
    for de in range(ne):
        for ds in range(n):
            if de or ds:
                send(
                    sq_src, sq_all.at[de * n + ds], sq_sem.at[0], sq_sem.at[1],
                    lax.rem(me + ds, n), lax.rem(ex + de, ne),
                )
    own(g_nxt, every[2:])
    if nz > 1:
        relay(g_nxt, 1, every[:1])
    loads[5].wait()
    loads[6].wait()
    await_copy(sq_all.at[pl.ds(1, ne * n - 1)], sq_sem.at[1])
    norm = sq_src[...]
    for k in range(1, ne * n):
        norm = norm + sq_all[k]
    rms = jnp.sqrt(jnp.sum(norm, keepdims=True) / entries + 1e-06)
    clip = jnp.minimum(1.0, 1.0 / rms)

    u_tile = 32
    first_scale, later_scale = 1.0 / (1.0 - 0.9**10), 1.0 / (1.0 - 0.999**10)

    def u_body(i, acc):
        rows = pl.ds(pl.multiple_of(i * u_tile, u_tile), u_tile)
        g = clip * w_out[rows, :]
        m_new = 0.9 * m_out[rows, :].astype(jnp.float32) + 0.1 * g
        v_new = 0.999 * v_out[rows, :].astype(jnp.float32) + 0.001 * g * g
        m_out[rows, :] = m_new.astype(jnp.bfloat16)
        v_out[rows, :] = v_new.astype(jnp.bfloat16)
        later = v_new * later_scale
        root = later * lax.rsqrt(later)
        u = (m_new * first_scale) / (root + 1e-06) + 0.01 * w[rows, :]
        w_out[rows, :] = u
        return acc + fold(u * u)

    def u_span(first, last, acc):
        return lax.fori_loop(first, last, u_body, acc)

    steps = d_blk // u_tile
    mid = steps // 2
    acc = u_span(0, mid, zero)
    if nz > 1:
        relay(g_nxt, 1, every[1:2])
    acc = u_span(mid, steps, acc)
    up_src[1:2] = jnp.sum(acc, axis=0, keepdims=True)
    for ds in range(1, n):
        send(up_src, up_all.at[ds], up_sem.at[0], up_sem.at[1], lax.rem(me + ds, n))
    if nz > 1:
        relay(g_nxt, 1, every[2:])
    if nz > 2:
        relay(g_nxt, 2, every[:2])
    await_copy(up_all.at[pl.ds(1, n - 1)], up_sem.at[1])
    sums = up_src[...]
    for ds in range(1, n):
        sums = sums + up_all[ds]
    trust = jnp.sqrt(jnp.sum(sums[0:1], keepdims=True)) / (jnp.sqrt(jnp.sum(sums[1:2], keepdims=True)) + 1e-06)
    rate = 0.08 * trust

    def p_body(i, carry):
        rows = pl.ds(pl.multiple_of(i * u_tile, u_tile), u_tile)
        x = w[rows, :] - rate * w_out[rows, :]
        w_out[rows, :] = x
        wb[rows, :] = x.astype(jnp.bfloat16)
        return carry

    lax.fori_loop(0, steps, p_body, 0)

    def crossed(t):
        for h in range(2 if t else 1):
            for d in range(1, nx):
                slot = lax.rem(iz - (1 - 2 * h) * t + nz, nz) * nx + lax.rem(ix - d + nx, nx)
                await_copy(nxt_all.at[slot], nx_recv.at[h, t, d - 1], holds(h, t) if t else None)

    def project(k, dx):
        peer = peer_to(k, dx)
        start = 0
        for piece in pieces:
            cols = pl.ds(start, piece)
            y = jnp.dot(nxt_all[peer], wb[:, cols], preferred_element_type=jnp.float32)
            cot_all[peer, :, cols] = y.astype(jnp.bfloat16)
            if dx or not (isinstance(k, int) and k == 0):
                mine = pl.ds(pl.multiple_of(me * f_blk + start, LANES), piece)
                send(cot_all.at[peer, :, cols], got.at[:, mine], y_sem.at[0], y_sem.at[1], peer)
            start += piece

    if nz == 4:
        project(ks[0], 0)
        relay(g_nxt, 2, every[2:])
        project(ks[1], 0)
        crossed(0)
        crossed(1)
        for dx in others:
            project(ks[0], dx)
        relay(g_nxt, 3, every)
        project(ks[2], 0)
        crossed(2)
        for dx in others:
            project(ks[1], dx)
        crossed(3)
        for dx in others:
            project(ks[2], dx)
    else:
        for t in range(2, nz):
            relay(g_nxt, t, every[2:] if t == 2 else every)
        for t in range(nz):
            crossed(t)
        for k in ks:
            for dx in range(nx):
                project(k, dx)
    for dx in others:
        project(0, dx)
    project(0, 0)
    got[:, pl.ds(pl.multiple_of(me * f_blk, LANES), f_blk)] = cot_all[me]
    if n > 1:
        await_copy(got.at[:, pl.ds(0, (n - 1) * f_blk)], y_sem.at[1])
        drains.append((got.at[:, pl.ds(0, (n - 1) * f_blk)], y_sem.at[0], None))
        drains.append((cot_all.at[pl.ds(0, n - 1)], cot_sem.at[0], None))
        drains.append((up_all.at[pl.ds(1, n - 1)], up_sem.at[0], None))
    drains.append((sq_all.at[pl.ds(1, ne * n - 1)], sq_sem.at[0], None))
    for ref, sem, when in drains:
        await_copy(ref, sem, when)


def fused_body(activations, out_grads, next_inputs, counts, master, moment, second):
    n = lax.axis_size("shard")
    ne = lax.axis_size("expert")
    cap, d_full = activations.shape[2:]
    ff = out_grads.shape[3]
    d_blk, f_blk = master.shape[2:]
    nx = columns_of(n)
    nz = n // nx
    entries = float(ne * master.shape[0] * d_full * ff)
    f32, bf16 = jnp.float32, jnp.bfloat16
    any_spec = pl.BlockSpec(memory_space=pl.ANY)
    vmem_spec = pl.BlockSpec(memory_space=pltpu.VMEM)
    dma = pltpu.SemaphoreType.DMA
    parts = 4
    pieces = split_lanes(f_blk, 2)
    strips = split_lanes(f_blk, 3)[::-1]
    across = dma((2, nz, max(nx - 1, 1)))
    results = pl.pallas_call(
        functools.partial(fused_kernel, n, ne, nx, entries, parts, strips, pieces),
        out_shape=(
            pltpu.VMEM((d_blk, f_blk), f32),
            pltpu.VMEM((d_blk, f_blk), bf16),
            pltpu.VMEM((d_blk, f_blk), bf16),
            pltpu.VMEM((cap, ff), bf16),
        ),
        in_specs=[pl.BlockSpec(memory_space=pltpu.HBM)] * 7,
        out_specs=(vmem_spec,) * 4,
        scratch_shapes=[
            pltpu.VMEM((n, cap, d_full), bf16),
            pltpu.VMEM((n, cap, d_full), bf16),
            pltpu.VMEM((n, cap, f_blk), bf16),
            pltpu.VMEM((cap, ff), bf16),
            pltpu.VMEM((d_blk, f_blk), f32),
            pltpu.VMEM((d_blk, f_blk), bf16),
            pltpu.VMEM((1, 1), jnp.int32),
            pltpu.VMEM((1, LANES), f32),
            pltpu.VMEM((ne * n, 1, LANES), f32),
            pltpu.VMEM((2, LANES), f32),
            pltpu.VMEM((n, 2, LANES), f32),
            dma((7,)),
        ]
        + [dma((2, nz)), dma((2, parts, nz)), across, dma((1,))]
        + [dma((2, nz)), dma((2, parts, nz)), across, across]
        + [dma((1 + len(strips),))] + [dma((2,))] * 3,
        compiler_params=pltpu.CompilerParams(
            collective_id=0, has_side_effects=True, vmem_limit_bytes=47 * 2**20
        ),
    )(counts, activations[0, 0], out_grads[0, 0], next_inputs[0, 0], master[0, 0], moment[0, 0], second[0, 0])
    outs = pl.pallas_call(
        store_kernel,
        out_shape=tuple(jax.ShapeDtypeStruct(x.shape, x.dtype) for x in results),
        in_specs=[vmem_spec] * 4,
        out_specs=(any_spec,) * 4,
        scratch_shapes=[dma((4,))],
        compiler_params=pltpu.CompilerParams(vmem_limit_bytes=2**20),
    )(*results)
    return tuple(x[None, None] for x in outs)


def body(activations, out_grads, next_inputs, counts, master, moment, second):
    n = lax.axis_size("shard")
    nz = n // columns_of(n)
    whole_rows = activations.shape[3] == master.shape[2]
    step = fused_body if whole_rows and nz & (nz - 1) == 0 else split_body
    return step(activations, out_grads, next_inputs, counts, master, moment, second)


def solution(mesh):
    spec = P("expert", "shard", None, None)
    return jax.shard_map(
        body,
        mesh=mesh,
        in_specs=(spec, spec, spec, P("expert", "shard"), spec, spec, spec),
        out_specs=(spec,) * 4,
        check_vma=False,
    )
```

```python
import functools
import jax
import jax.numpy as jnp
from jax import lax
from jax.experimental import pallas as pl
from jax.experimental.pallas import tpu as pltpu
from jax.sharding import PartitionSpec as P

MESH = pl.DeviceIdType.MESH
LANES = 128
SUBLANES = 8


def columns_of(n):
    nx = 1
    while n % (2 * nx) == 0 and 8 * nx * nx <= n:
        nx *= 2
    return nx


def fold(x):
    rows, cols = x.shape
    x = jnp.sum(x.reshape(rows // SUBLANES, SUBLANES, cols), axis=0)
    acc = x[:, 0:LANES]
    for c in range(LANES, cols, LANES):
        acc = acc + x[:, c : c + LANES]
    return acc


def greet(axes):
    barrier = pltpu.get_barrier_semaphore()
    total = 0
    for name, size in axes:
        mine = lax.axis_index(name)
        for d in range(1, size):
            peer = lax.rem(mine + d, size)
            pl.semaphore_signal(barrier, inc=1, device_id={name: peer}, device_id_type=MESH)
        total += size - 1
    pl.semaphore_wait(barrier, total)


def step_kernel(
    n, ne, nx, grid_c, entries,
    act, cots, nxt, w_hbm, m_hbm, v_hbm,
    w_out, m_out, v_out, wb_out, nxt_all,
    acts, cot_all, w, m, v, sq_src, sq_all, ex_src, ex_all, up_src, up_all,
    load_sem, own_sem,
    az_send, az_recv, ax_send, ax_recv, nz_send, nz_recv, nx_send, nx_recv,
    cot_send, cot_recv, sq_send, sq_recv, ex_send, ex_recv, up_send, up_recv,
):
    nz = n // nx
    me = lax.axis_index("shard")
    ex = lax.axis_index("expert")
    iz, ix = me // nx, lax.rem(me, nx)
    cap, d_full = act.shape
    d_blk, f_blk = w.shape
    half = cap // 2
    row0 = pl.multiple_of((me // grid_c) * d_blk, d_blk)

    loads = [
        pltpu.make_async_copy(src, dst, load_sem.at[i])
        for i, (src, dst) in enumerate(((w_hbm, w), (m_hbm, m), (v_hbm, v)))
    ]
    owns = [
        pltpu.make_async_copy(act, acts.at[me], own_sem.at[0]),
        pltpu.make_async_copy(nxt, nxt_all.at[me], own_sem.at[1]),
        pltpu.make_async_copy(cots.at[lax.rem(me, grid_c)], cot_all.at[me], own_sem.at[2]),
    ]
    for c in owns + loads:
        c.start()
    greet((("shard", n), ("expert", ne)))
    owns[0].wait()
    owns[1].wait()

    sends = []

    def send(src, dst, s, r, peer, axis="shard", when=None):
        c = pltpu.make_async_remote_copy(
            src_ref=src, dst_ref=dst, send_sem=s, recv_sem=r,
            device_id={axis: peer}, device_id_type=MESH,
        )
        if when is None:
            c.start()
        else:
            pl.when(when)(c.start)
        sends.append((when, c))

    def z_slot(k):
        return lax.rem(iz + k + nz, nz) * nx + ix

    def part(buf, slot, p):
        return buf.at[slot, pl.ds(p * half, half)]

    def holds(h, t):
        return iz >= t if h == 0 else iz < nz - t

    def z_send(buf, t, h, p, zs, zr):
        way = 1 - 2 * h
        slot = z_slot(-way * (t - 1))
        more = jnp.logical_and(iz >= t - 1, iz < nz - 1) if h == 0 else jnp.logical_and(iz <= nz - t, iz > 0)
        send(part(buf, slot, p), part(buf, slot, p), zs.at[h, p, t], zr.at[h, p, t], z_slot(way), when=more)

    def x_send(buf, t, h, p, xs, xr):
        way = 1 - 2 * h
        slot = z_slot(-way * t)
        for d in range(1, nx):
            peer = iz * nx + lax.rem(ix + d, nx)
            send(
                part(buf, slot, p), part(buf, slot, p), xs.at[h, p, t, d], xr.at[h, p, t, d], peer,
                when=None if t == 0 else holds(h, t),
            )

    def arrived(buf, slot, p, sem, when=None):
        ref = part(buf, slot, p)
        c = pltpu.make_async_copy(ref, ref, sem)
        if when is None:
            c.wait()
        else:
            pl.when(when)(c.wait)

    def own_sends(buf, zs, zr, xs, xr):
        for p in range(2):
            if nz > 1:
                for h in range(2):
                    z_send(buf, 1, h, p, zs, zr)
            x_send(buf, 0, 0, p, xs, xr)

    def relay(buf, t, zs, zr, xs, xr):
        for p in range(2):
            for h in range(2):
                arrived(buf, z_slot(-(1 - 2 * h) * t), p, zr.at[h, p, t], when=holds(h, t))
                if t < nz - 1:
                    z_send(buf, t + 1, h, p, zs, zr)
                x_send(buf, t, h, p, xs, xr)

    def finish(buf, xr):
        for t in range(nz):
            for h in range(2 if t else 1):
                for p in range(2):
                    for d in range(1, nx):
                        slot = lax.rem(iz - (1 - 2 * h) * t + nz, nz) * nx + lax.rem(ix - d + nx, nx)
                        arrived(buf, slot, p, xr.at[h, p, t, d], when=holds(h, t) if t else None)

    def cot_sends(ds):
        for d in ds:
            peer = lax.rem(me + d, n)
            send(cots.at[lax.rem(peer, grid_c)], cot_all.at[me], cot_send.at[d], cot_recv.at[d], peer)

    acts_sems = (az_send, az_recv, ax_send, ax_recv)
    nxt_sems = (nz_send, nz_recv, nx_send, nx_recv)
    own_sends(acts, *acts_sems)
    order = sorted(range(1, n), key=lambda d: -min(d, n - d))
    share = -(-len(order) // nz)
    cot_sends(order[:share])
    for t in range(1, nz):
        relay(acts, t, *acts_sems)
        cot_sends(order[share * t : share * (t + 1)])
    own_sends(nxt_all, *nxt_sems)

    tile = 64
    loads[0].wait()

    def w_body(i, acc):
        x = w[pl.ds(i * tile, tile), :]
        return acc + fold(x * x)

    zero = jnp.zeros((SUBLANES, LANES), jnp.float32)
    up_src[0] = lax.fori_loop(0, d_blk // tile, w_body, zero)
    loads[1].wait()
    loads[2].wait()
    finish(acts, ax_recv)
    owns[2].wait()
    for d in range(1, n):
        slot = lax.rem(me - d + n, n)
        pltpu.make_async_copy(cot_all.at[slot], cot_all.at[slot], cot_recv.at[d]).wait()

    g_tile = 256

    def g_body(i, acc):
        a = acts[:, :, pl.ds(pl.multiple_of(row0 + i * g_tile, g_tile), g_tile)]
        g = lax.dot_general(
            a.reshape(n * cap, g_tile), cot_all[...].reshape(n * cap, f_blk),
            (((0,), (0,)), ((), ())), preferred_element_type=jnp.float32,
        )
        w_out[pl.ds(pl.multiple_of(i * g_tile, g_tile), g_tile), :] = g
        return acc + fold(g * g)

    sq_src[...] = lax.fori_loop(0, d_blk // g_tile, g_body, zero)

    def spread(src, dst, ss, rs, axis, mine, size):
        for d in range(1, size):
            send(src, dst.at[mine], ss.at[d], rs.at[d], lax.rem(mine + d, size), axis)

    def collect(src, dst, rs, mine, size):
        total = src[...]
        for d in range(1, size):
            slot = lax.rem(mine - d + size, size)
            pltpu.make_async_copy(dst.at[slot], dst.at[slot], rs.at[d]).wait()
            total = total + dst[slot]
        return total

    spread(sq_src, sq_all, sq_send, sq_recv, "shard", me, n)
    if nz > 1:
        relay(nxt_all, 1, *nxt_sems)
    ex_src[...] = collect(sq_src, sq_all, sq_recv, me, n)
    spread(ex_src, ex_all, ex_send, ex_recv, "expert", ex, ne)
    norm_total = jnp.sum(collect(ex_src, ex_all, ex_recv, ex, ne), keepdims=True)
    rms = jnp.sqrt(norm_total / entries + 1e-06)
    clip = jnp.minimum(1.0, 1.0 / rms)
    for t in range(2, nz):
        if t < nz - 1:
            relay(nxt_all, t, *nxt_sems)

    u_tile = 32

    def u_body(i, acc):
        rows = pl.ds(pl.multiple_of(i * u_tile, u_tile), u_tile)
        g = clip * w_out[rows, :]
        m_new = 0.9 * m[rows, :].astype(jnp.float32) + 0.1 * g
        v_new = 0.999 * v[rows, :].astype(jnp.float32) + 0.001 * g * g
        m_out[rows, :] = m_new.astype(jnp.bfloat16)
        v_out[rows, :] = v_new.astype(jnp.bfloat16)
        scaled = m_new * (1.0 / (1.0 - 0.9**10))
        root = jnp.sqrt(v_new * (1.0 / (1.0 - 0.999**10)))
        u = scaled / (root + 1e-06) + 0.01 * w[rows, :]
        w_out[rows, :] = u
        return acc + fold(u * u)

    up_src[1] = lax.fori_loop(0, d_blk // u_tile, u_body, zero)
    spread(up_src, up_all, up_send, up_recv, "shard", me, n)
    if nz > 2:
        relay(nxt_all, nz - 1, *nxt_sems)
    sums = collect(up_src, up_all, up_recv, me, n)
    trust = jnp.sqrt(jnp.sum(sums[0], keepdims=True)) / (
        jnp.sqrt(jnp.sum(sums[1], keepdims=True)) + 1e-06
    )
    rate = 0.08 * trust

    def p_body(i, carry):
        rows = pl.ds(pl.multiple_of(i * u_tile, u_tile), u_tile)
        x = w[rows, :] - rate * w_out[rows, :]
        w_out[rows, :] = x
        wb_out[rows, :] = x.astype(jnp.bfloat16)
        return carry

    lax.fori_loop(0, d_blk // u_tile, p_body, 0)
    finish(nxt_all, nx_recv)
    for when, c in sends:
        if when is None:
            c.wait_send()
        else:
            pl.when(when)(c.wait_send)


def project_kernel(n, grid_c, chunks, nxt_all, wb, got, made, own_sem, send_sem, recv_sem):
    me = lax.axis_index("shard")
    d_blk, f_blk = wb.shape
    cap = nxt_all.shape[1]
    row0 = pl.multiple_of((me // grid_c) * d_blk, d_blk)
    greet((("shard", n),))
    copies = []
    start = 0
    for k, width in enumerate(chunks):
        cols = pl.ds(start, width)
        x = nxt_all[:, :, pl.ds(row0, d_blk)].reshape(n * cap, d_blk)
        y = jnp.dot(x, wb[:, cols], preferred_element_type=jnp.float32)
        made[:, :, cols] = y.astype(made.dtype).reshape(n, cap, width)
        for d in range(1, n):
            peer = lax.rem(me + d, n)
            c = pltpu.make_async_remote_copy(
                src_ref=made.at[peer, :, cols], dst_ref=got.at[me, :, cols],
                send_sem=send_sem.at[k, d], recv_sem=recv_sem.at[k, d],
                device_id={"shard": peer}, device_id_type=MESH,
            )
            c.start()
            copies.append(c)
        start += width
    own = pltpu.make_async_copy(made.at[me], got.at[me], own_sem.at[0])
    own.start()
    own.wait()
    start = 0
    for k, width in enumerate(chunks):
        for d in range(1, n):
            ref = got.at[lax.rem(me - d + n, n), :, pl.ds(start, width)]
            pltpu.make_async_copy(ref, ref, recv_sem.at[k, d]).wait()
        start += width
    for c in copies:
        c.wait_send()


def store_kernel(*refs):
    count = len(refs) // 2
    sems = refs[-1]
    copies = [pltpu.make_async_copy(refs[i], refs[count + i], sems.at[i]) for i in range(count)]
    for c in copies:
        c.start()
    for c in copies:
        c.wait()


def split_lanes(f_blk, parts):
    units = f_blk // LANES
    parts = min(parts, units)
    return tuple((units // parts + (1 if i >= parts - units % parts else 0)) * LANES for i in range(parts))


def split_body(activations, out_grads, next_inputs, counts, master, moment, second):
    n = lax.axis_size("shard")
    ne = lax.axis_size("expert")
    cap, d_full = activations.shape[2:]
    ff = out_grads.shape[3]
    d_blk, f_blk = master.shape[2:]
    grid_r, grid_c = d_full // d_blk, ff // f_blk
    nx = columns_of(n)
    nz = n // nx
    entries = float(ne * master.shape[0] * d_full * ff)
    valid = lax.iota(jnp.int32, cap) < counts[0, 0]
    masked = jnp.where(valid[:, None], out_grads[0, 0], jnp.zeros((), jnp.bfloat16))
    cots = masked.reshape(cap, grid_c, f_blk).transpose(1, 0, 2)

    f32, bf16 = jnp.float32, jnp.bfloat16
    any_spec = pl.BlockSpec(memory_space=pl.ANY)
    vmem_spec = pl.BlockSpec(memory_space=pltpu.VMEM)
    dma = pltpu.SemaphoreType.DMA
    sq = (SUBLANES, LANES)
    w_new, m_new, v_new, wb, nxt_all = pl.pallas_call(
        functools.partial(step_kernel, n, ne, nx, grid_c, entries),
        out_shape=(
            pltpu.VMEM((d_blk, f_blk), f32),
            pltpu.VMEM((d_blk, f_blk), bf16),
            pltpu.VMEM((d_blk, f_blk), bf16),
            pltpu.VMEM((d_blk, f_blk), bf16),
            pltpu.VMEM((n, cap, d_full), bf16),
        ),
        in_specs=[any_spec] * 3 + [pl.BlockSpec(memory_space=pltpu.HBM)] * 3,
        out_specs=(vmem_spec,) * 5,
        scratch_shapes=[
            pltpu.VMEM((n, cap, d_full), bf16),
            pltpu.VMEM((n, cap, f_blk), bf16),
            pltpu.VMEM((d_blk, f_blk), f32),
            pltpu.VMEM((d_blk, f_blk), bf16),
            pltpu.VMEM((d_blk, f_blk), bf16),
            pltpu.VMEM(sq, f32),
            pltpu.VMEM((n,) + sq, f32),
            pltpu.VMEM(sq, f32),
            pltpu.VMEM((ne,) + sq, f32),
            pltpu.VMEM((2,) + sq, f32),
            pltpu.VMEM((n, 2) + sq, f32),
            dma((3,)),
            dma((3,)),
        ]
        + [dma((2, 2, nz)), dma((2, 2, nz)), dma((2, 2, nz, nx)), dma((2, 2, nz, nx))] * 2
        + [dma((n,)), dma((n,)), dma((n,)), dma((n,)), dma((ne,)), dma((ne,)), dma((n,)), dma((n,))],
        compiler_params=pltpu.CompilerParams(
            collective_id=0, has_side_effects=True, vmem_limit_bytes=26 * 2**20
        ),
    )(activations[0, 0], cots, next_inputs[0, 0], master[0, 0], moment[0, 0], second[0, 0])

    w_new, m_new, v_new = pl.pallas_call(
        store_kernel,
        out_shape=tuple(jax.ShapeDtypeStruct(x.shape, x.dtype) for x in (w_new, m_new, v_new)),
        in_specs=[vmem_spec] * 3,
        out_specs=(any_spec,) * 3,
        scratch_shapes=[dma((3,))],
        compiler_params=pltpu.CompilerParams(vmem_limit_bytes=2**20),
    )(w_new, m_new, v_new)

    back = bf16 if grid_r == 1 else f32
    chunks = split_lanes(f_blk, 3)
    got = pl.pallas_call(
        functools.partial(project_kernel, n, grid_c, chunks),
        out_shape=jax.ShapeDtypeStruct((n, cap, f_blk), back),
        in_specs=[vmem_spec] * 2,
        out_specs=vmem_spec,
        scratch_shapes=[
            pltpu.VMEM((n, cap, f_blk), back),
            dma((1,)),
            dma((len(chunks), n)),
            dma((len(chunks), n)),
        ],
        compiler_params=pltpu.CompilerParams(
            collective_id=1, has_side_effects=True, vmem_limit_bytes=16 * 2**20
        ),
    )(nxt_all, wb)
    summed = jnp.sum(got.reshape(grid_r, grid_c, cap, f_blk), axis=0)
    projected = summed.transpose(1, 0, 2).reshape(cap, ff).astype(bf16)
    return w_new[None, None], m_new[None, None], v_new[None, None], projected[None, None]


def flip(z, k, top):
    out, bit = z, 1
    while bit < top:
        out = out + lax.rem(lax.div(k, bit), 2) * bit * (1 - 2 * lax.rem(lax.div(z, bit), 2))
        bit *= 2
    return out


def fused_kernel(
    n, ne, nx, entries, parts, strips, pieces,
    cnt_hbm, act, cot_hbm, nxt, w_hbm, m_hbm, v_hbm,
    w_out, m_out, v_out, got,
    acts, nxt_all, cot_all, cots, w, wb, cnt, sq_src, sq_all, up_src, up_all,
    load_sem,
    az_send, az_recv, ax_send, ax_recv, nz_send, nz_recv, nx_send, nx_recv,
    cot_sem, sq_sem, up_sem, y_sem,
):
    nz = n // nx
    me = lax.axis_index("shard")
    ex = lax.axis_index("expert")
    iz, ix = lax.div(me, nx), lax.rem(me, nx)
    cap, d_full = act.shape
    d_blk, f_blk = w.shape

    barrier = pltpu.get_barrier_semaphore()
    for de in range(ne):
        for ds in range(n):
            if de or ds:
                pl.semaphore_signal(
                    barrier, inc=1, device_id_type=MESH,
                    device_id={"expert": lax.rem(ex + de, ne), "shard": lax.rem(me + ds, n)},
                )
    loads = [
        pltpu.make_async_copy(src, dst, load_sem.at[i])
        for i, (src, dst) in enumerate((
            (cnt_hbm, cnt), (act, acts.at[me]), (cot_hbm, cots), (nxt, nxt_all.at[me]),
            (w_hbm, w), (m_hbm, m_out), (v_hbm, v_out),
        ))
    ]
    for c in loads:
        c.start()
    loads[0].wait()
    loads[1].wait()
    loads[2].wait()
    valid = lax.broadcasted_iota(jnp.int32, (cap, f_blk), 0) < cnt[...]

    def mask_body(j, carry):
        cols = pl.ds(pl.multiple_of(j * f_blk, LANES), f_blk)
        x = cots[:, cols].astype(jnp.float32)
        cots[:, cols] = jnp.where(valid, x, 0.0).astype(jnp.bfloat16)
        return carry

    lax.fori_loop(0, n, mask_body, 0)
    pl.semaphore_wait(barrier, ne * n - 1)

    drains = []

    def send(src, dst, s, r, shard, expert=None, when=None):
        device = {"shard": shard} if expert is None else {"expert": expert, "shard": shard}
        c = pltpu.make_async_remote_copy(
            src_ref=src, dst_ref=dst, send_sem=s, recv_sem=r, device_id=device, device_id_type=MESH,
        )
        if when is None:
            c.start()
        else:
            pl.when(when)(c.start)

    def await_copy(ref, sem, when=None):
        c = pltpu.make_async_copy(ref, ref, sem)
        if when is None:
            c.wait()
        else:
            pl.when(when)(c.wait)

    def z_slot(k):
        return lax.rem(iz + k + nz, nz) * nx + ix

    def cut(buf, slot, p):
        width = d_full // parts
        return buf.at[slot, :, pl.ds(p * width, width)]

    def holds(h, t):
        return iz >= t if h == 0 else iz < nz - t

    def z_send(g, t, h, p):
        buf, zs, zr, _, _ = g
        way = 1 - 2 * h
        slot = z_slot(-way * (t - 1))
        more = jnp.logical_and(iz >= t - 1, iz < nz - 1) if h == 0 else jnp.logical_and(iz <= nz - t, iz > 0)
        block = cut(buf, slot, p)
        send(block, block, zs.at[h, t], zr.at[h, p, t], z_slot(way), when=more)
        if p == 0:
            drains.append((buf.at[slot], zs.at[h, t], more))

    def x_send(g, t, h, p):
        buf, _, _, xs, xr = g
        slot = z_slot(-(1 - 2 * h) * t)
        when = None if t == 0 else holds(h, t)
        block = cut(buf, slot, p)
        for d in range(1, nx):
            landing = xr.at[0] if buf is acts else xr.at[h, t, d - 1]
            send(block, block, xs.at[h, t, d - 1], landing, iz * nx + lax.rem(ix + d, nx), when=when)
            if p == 0:
                drains.append((buf.at[slot], xs.at[h, t, d - 1], when))

    def own(g, ps):
        for p in ps:
            if nz > 1:
                for h in range(2):
                    z_send(g, 1, h, p)
            x_send(g, 0, 0, p)

    def relay(g, t, ps):
        for p in ps:
            for h in range(2):
                await_copy(cut(g[0], z_slot(-(1 - 2 * h) * t), p), g[2].at[h, p, t], holds(h, t))
                if t < nz - 1:
                    z_send(g, t + 1, h, p)
                x_send(g, t, h, p)

    def peer_to(k, dx):
        return flip(iz, k, nz) * nx + lax.rem(ix + dx, nx)

    def cot_send(k, dx, q):
        peer = peer_to(k, dx)
        start, span = sum(strips[:q]), strips[q]
        cols = pl.ds(pl.multiple_of(peer * f_blk + start, LANES), span)
        send(cots.at[:, cols], cot_all.at[me, :, pl.ds(start, span)], cot_sem.at[0], cot_sem.at[1 + q], peer)

    g_acts = (acts, az_send, az_recv, ax_send, ax_recv)
    g_nxt = (nxt_all, nz_send, nz_recv, nx_send, nx_recv)
    every = range(parts)
    tile = 64

    def w_body(i, acc):
        x = w[pl.ds(pl.multiple_of(i * tile, tile), tile), :]
        return acc + fold(x * x)

    zero = jnp.zeros((SUBLANES, LANES), jnp.float32)
    if nz == 4:
        inner = lax.rem(lax.div(iz + 1, 2), 2)
        ks = [1 + 2 * inner, 2, 3 - 2 * inner]
    else:
        ks = sorted(range(1, nz), key=lambda k: (-k.bit_length(), k))
    others = range(1, nx)

    def exchange(k, q):
        for dx in range(nx):
            cot_send(k, dx, q)

    def near(q):
        for dx in others:
            cot_send(0, dx, q)

    own(g_acts, every)
    if nz > 1:
        relay(g_acts, 1, every)
        exchange(ks[0], 0)
    cot_all[me] = cots[:, pl.ds(pl.multiple_of(me * f_blk, LANES), f_blk)]
    loads[4].wait()
    squares = lax.fori_loop(0, d_blk // tile, w_body, zero)
    for t in range(2, nz - 1):
        relay(g_acts, t, every)
    for k in ks[1:]:
        exchange(k, 0)
    near(0)
    if nz > 2:
        relay(g_acts, nz - 1, every)
    for q in range(1, len(strips)):
        for k in ks:
            exchange(k, q)
        near(q)
    loads[3].wait()
    own(g_nxt, every[:2])
    up_src[0:1] = jnp.sum(squares, axis=0, keepdims=True)

    g_tile = min(1024, d_blk)

    if nx > 1:
        await_copy(acts.at[pl.ds(0, nz * (nx - 1))], ax_recv.at[0])
    total = zero
    for q, span in enumerate(strips):
        cols = pl.ds(sum(strips[:q]), span)
        await_copy(cot_all.at[pl.ds(0, n - 1), :, cols], cot_sem.at[1 + q])

        def g_body(i, acc):
            rows = pl.ds(pl.multiple_of(i * g_tile, g_tile), g_tile)
            g = lax.dot_general(
                acts[:, :, rows].reshape(n * cap, g_tile), cot_all[:, :, cols].reshape(n * cap, span),
                (((0,), (0,)), ((), ())), preferred_element_type=jnp.float32,
            )
            w_out[rows, cols] = g
            return acc + fold(g * g)

        total = lax.fori_loop(0, d_blk // g_tile, g_body, total)
    sq_src[...] = jnp.sum(total, axis=0, keepdims=True)
    for de in range(ne):
        for ds in range(n):
            if de or ds:
                send(
                    sq_src, sq_all.at[de * n + ds], sq_sem.at[0], sq_sem.at[1],
                    lax.rem(me + ds, n), lax.rem(ex + de, ne),
                )
    own(g_nxt, every[2:])
    if nz > 1:
        relay(g_nxt, 1, every[:1])
    loads[5].wait()
    loads[6].wait()
    await_copy(sq_all.at[pl.ds(1, ne * n - 1)], sq_sem.at[1])
    norm = sq_src[...]
    for k in range(1, ne * n):
        norm = norm + sq_all[k]
    rms = jnp.sqrt(jnp.sum(norm, keepdims=True) / entries + 1e-06)
    clip = jnp.minimum(1.0, 1.0 / rms)

    u_tile = 64
    first_scale, later_scale = 1.0 / (1.0 - 0.9**10), 1.0 / (1.0 - 0.999**10)

    def u_body(i, acc):
        rows = pl.ds(pl.multiple_of(i * u_tile, u_tile), u_tile)
        g = clip * w_out[rows, :]
        m_new = 0.9 * m_out[rows, :].astype(jnp.float32) + 0.1 * g
        v_new = 0.999 * v_out[rows, :].astype(jnp.float32) + 0.001 * g * g
        m_out[rows, :] = m_new.astype(jnp.bfloat16)
        v_out[rows, :] = v_new.astype(jnp.bfloat16)
        later = v_new * later_scale
        root = later * lax.rsqrt(later)
        u = (m_new * first_scale) / (root + 1e-06) + 0.01 * w[rows, :]
        w_out[rows, :] = u
        return acc + fold(u * u)

    def u_span(first, last, acc):
        return lax.fori_loop(first, last, u_body, acc)

    steps = d_blk // u_tile
    mid = steps // 2
    acc = u_span(0, mid, zero)
    if nz > 1:
        relay(g_nxt, 1, every[1:2])
    acc = u_span(mid, steps, acc)
    up_src[1:2] = jnp.sum(acc, axis=0, keepdims=True)
    for ds in range(1, n):
        send(up_src, up_all.at[ds], up_sem.at[0], up_sem.at[1], lax.rem(me + ds, n))
    if nz > 1:
        relay(g_nxt, 1, every[2:])
    if nz > 2:
        relay(g_nxt, 2, every[:2])
    await_copy(up_all.at[pl.ds(1, n - 1)], up_sem.at[1])
    sums = up_src[...]
    for ds in range(1, n):
        sums = sums + up_all[ds]
    trust = jnp.sqrt(jnp.sum(sums[0:1], keepdims=True)) / (jnp.sqrt(jnp.sum(sums[1:2], keepdims=True)) + 1e-06)
    rate = 0.08 * trust

    def p_body(i, carry):
        rows = pl.ds(pl.multiple_of(i * u_tile, u_tile), u_tile)
        x = w[rows, :] - rate * w_out[rows, :]
        w_out[rows, :] = x
        wb[rows, :] = x.astype(jnp.bfloat16)
        return carry

    lax.fori_loop(0, steps, p_body, 0)

    def crossed(t):
        for h in range(2 if t else 1):
            for d in range(1, nx):
                slot = lax.rem(iz - (1 - 2 * h) * t + nz, nz) * nx + lax.rem(ix - d + nx, nx)
                await_copy(nxt_all.at[slot], nx_recv.at[h, t, d - 1], holds(h, t) if t else None)

    def project(k, dx):
        peer = peer_to(k, dx)
        start = 0
        for piece in pieces:
            cols = pl.ds(start, piece)
            y = jnp.dot(nxt_all[peer], wb[:, cols], preferred_element_type=jnp.float32)
            cot_all[peer, :, cols] = y.astype(jnp.bfloat16)
            if dx or not (isinstance(k, int) and k == 0):
                mine = pl.ds(pl.multiple_of(me * f_blk + start, LANES), piece)
                send(cot_all.at[peer, :, cols], got.at[:, mine], y_sem.at[0], y_sem.at[1], peer)
            start += piece

    if nz == 4:
        project(ks[0], 0)
        relay(g_nxt, 2, every[2:])
        project(ks[1], 0)
        crossed(0)
        crossed(1)
        for dx in others:
            project(ks[0], dx)
        relay(g_nxt, 3, every)
        project(ks[2], 0)
        crossed(2)
        for dx in others:
            project(ks[1], dx)
        crossed(3)
        for dx in others:
            project(ks[2], dx)
    else:
        for t in range(2, nz):
            relay(g_nxt, t, every[2:] if t == 2 else every)
        for t in range(nz):
            crossed(t)
        for k in ks:
            for dx in range(nx):
                project(k, dx)
    for dx in others:
        project(0, dx)
    project(0, 0)
    got[:, pl.ds(pl.multiple_of(me * f_blk, LANES), f_blk)] = cot_all[me]
    if n > 1:
        await_copy(got.at[:, pl.ds(0, (n - 1) * f_blk)], y_sem.at[1])
        drains.append((got.at[:, pl.ds(0, (n - 1) * f_blk)], y_sem.at[0], None))
        drains.append((cot_all.at[pl.ds(0, n - 1)], cot_sem.at[0], None))
        drains.append((up_all.at[pl.ds(1, n - 1)], up_sem.at[0], None))
    drains.append((sq_all.at[pl.ds(1, ne * n - 1)], sq_sem.at[0], None))
    for ref, sem, when in drains:
        await_copy(ref, sem, when)


def fused_body(activations, out_grads, next_inputs, counts, master, moment, second):
    n = lax.axis_size("shard")
    ne = lax.axis_size("expert")
    cap, d_full = activations.shape[2:]
    ff = out_grads.shape[3]
    d_blk, f_blk = master.shape[2:]
    nx = columns_of(n)
    nz = n // nx
    entries = float(ne * master.shape[0] * d_full * ff)
    f32, bf16 = jnp.float32, jnp.bfloat16
    any_spec = pl.BlockSpec(memory_space=pl.ANY)
    vmem_spec = pl.BlockSpec(memory_space=pltpu.VMEM)
    dma = pltpu.SemaphoreType.DMA
    parts = 4
    pieces = split_lanes(f_blk, 2)
    strips = split_lanes(f_blk, 3)[::-1]
    across = dma((2, nz, max(nx - 1, 1)))
    results = pl.pallas_call(
        functools.partial(fused_kernel, n, ne, nx, entries, parts, strips, pieces),
        out_shape=(
            pltpu.VMEM((d_blk, f_blk), f32),
            pltpu.VMEM((d_blk, f_blk), bf16),
            pltpu.VMEM((d_blk, f_blk), bf16),
            pltpu.VMEM((cap, ff), bf16),
        ),
        in_specs=[pl.BlockSpec(memory_space=pltpu.HBM)] * 7,
        out_specs=(vmem_spec,) * 4,
        scratch_shapes=[
            pltpu.VMEM((n, cap, d_full), bf16),
            pltpu.VMEM((n, cap, d_full), bf16),
            pltpu.VMEM((n, cap, f_blk), bf16),
            pltpu.VMEM((cap, ff), bf16),
            pltpu.VMEM((d_blk, f_blk), f32),
            pltpu.VMEM((d_blk, f_blk), bf16),
            pltpu.VMEM((1, 1), jnp.int32),
            pltpu.VMEM((1, LANES), f32),
            pltpu.VMEM((ne * n, 1, LANES), f32),
            pltpu.VMEM((2, LANES), f32),
            pltpu.VMEM((n, 2, LANES), f32),
            dma((7,)),
        ]
        + [dma((2, nz)), dma((2, parts, nz)), across, dma((1,))]
        + [dma((2, nz)), dma((2, parts, nz)), across, across]
        + [dma((1 + len(strips),))] + [dma((2,))] * 3,
        compiler_params=pltpu.CompilerParams(
            collective_id=0, has_side_effects=True, vmem_limit_bytes=47 * 2**20
        ),
    )(counts, activations[0, 0], out_grads[0, 0], next_inputs[0, 0], master[0, 0], moment[0, 0], second[0, 0])
    outs = pl.pallas_call(
        store_kernel,
        out_shape=tuple(jax.ShapeDtypeStruct(x.shape, x.dtype) for x in results),
        in_specs=[vmem_spec] * 4,
        out_specs=(any_spec,) * 4,
        scratch_shapes=[dma((4,))],
        compiler_params=pltpu.CompilerParams(vmem_limit_bytes=2**20),
    )(*results)
    return tuple(x[None, None] for x in outs)


def body(activations, out_grads, next_inputs, counts, master, moment, second):
    n = lax.axis_size("shard")
    nz = n // columns_of(n)
    whole_rows = activations.shape[3] == master.shape[2]
    step = fused_body if whole_rows and nz & (nz - 1) == 0 else split_body
    return step(activations, out_grads, next_inputs, counts, master, moment, second)


def solution(mesh):
    spec = P("expert", "shard", None, None)
    return jax.shard_map(
        body,
        mesh=mesh,
        in_specs=(spec, spec, spec, P("expert", "shard"), spec, spec, spec),
        out_specs=(spec,) * 4,
        check_vma=False,
    )
```
